128 devices in a mesh: leaf: 16 (over y, z_hi, core), seq: 8 (over z_lo, x).
Axes of the slice: x: 4, y: 4, z: 4 (z_hi: 2, z_lo: 2; z = z_hi * 2 + z_lo), core: 2. Of those that a mesh axis runs over, the one named last changes fastest.
Arguments:
- prompt_q: bfloat16 [16, 1024, 1792], P('leaf', 'seq'), may hold values from -6 to 6
- prompt_k: bfloat16 [16, 1024, 256], P('leaf', 'seq'), may hold values from -6 to 6
- prompt_value_rows: bfloat16 [16, 1024, 256], P('leaf', 'seq'), may hold values from -6 to 6
- leaf_q: bfloat16 [16, 384, 1792], P('leaf', 'seq'), may hold values from -6 to 6
- leaf_k: bfloat16 [16, 384, 256], P('leaf', 'seq'), may hold values from -6 to 6
- leaf_value_rows: bfloat16 [16, 384, 256], P('leaf', 'seq'), may hold values from -6 to 6
- prompt_dy: bfloat16 [16, 1024, 3584], P('leaf', 'seq'), may hold values from -6 to 6
- leaf_dy: bfloat16 [16, 384, 3584], P('leaf', 'seq'), may hold values from -6 to 6
- out_weight: bfloat16 [1792, 3584], replicated, may hold values from -0.125 to 0.125
- lengths: int32 [16, 16], P('leaf'), may hold values from 1 to 48, 384 in all within a row
- offsets: int32 [16, 16], P('leaf'), may hold values from 1 to 1024
- parents: int32 [16, 16], P('leaf'), may hold values from 0 to 15, as said below
Outputs:
- prompt_dq: float32 [16, 1024, 1792], P('leaf', 'seq')
- prompt_dk: float32 [16, 1024, 256], P('leaf', 'seq')
- prompt_dv: float32 [16, 1024, 256], P('leaf', 'seq')
- leaf_dq: float32 [16, 384, 1792], P('leaf', 'seq')
- leaf_dk: float32 [16, 384, 256], P('leaf', 'seq')
- leaf_dv: float32 [16, 384, 256], P('leaf', 'seq')
- weight_grad: float32 [1792, 3584], P(('leaf', 'seq'))
The draws below stay inside these ranges and needn't reach their ends.
Inputs may be any that keep to these rules, and one draw needn't show every extreme that they name: parents[t, b] lies in 0 to b; the value b means that branch b has no ancestor branch.
All inputs are finite; a program needn't handle non-finite values.
Results may differ from the reference program's by a relative error of at most 0.025.
Values may be sent and summed in bfloat16 or wider, within the bound.
A program may use at most 128 MiB of HBM per device.

```python
import math
import jax
import jax.numpy as jnp
import numpy as np
from jax import lax

D = 3584
HEAD_SIZE = 128
QUERY_HEADS = 14
KEY_VALUE_HEADS = 2
QUERY_PER_KV = 7
BRANCHES = 16
SEARCH_TREES = 16
PROMPT_TOKENS = 1024
LEAF_TOKENS = 384
MOSTLEN = 48


def simple_sample(key, shape):
    return jnp.clip(jax.random.normal(jax.random.fold_in(key, 6), shape), -4.0, 4.0)


def draw_prompt_q(key, part):
    sampled_values = simple_sample(jax.random.fold_in(key, 13), (SEARCH_TREES, PROMPT_TOKENS, QUERY_HEADS * HEAD_SIZE))
    return sampled_values.astype(jnp.bfloat16)


def draw_prompt_k(key, part):
    sampled_values = simple_sample(jax.random.fold_in(key, 12), (SEARCH_TREES, PROMPT_TOKENS, KEY_VALUE_HEADS * HEAD_SIZE))
    return sampled_values.astype(jnp.bfloat16)


def draw_leaf_q(key, part):
    sampled_values = simple_sample(jax.random.fold_in(key, 15), (SEARCH_TREES, LEAF_TOKENS, QUERY_HEADS * HEAD_SIZE))
    return sampled_values.astype(jnp.bfloat16)


def draw_leaf_k(key, part):
    sampled_values = simple_sample(jax.random.fold_in(key, 14), (SEARCH_TREES, LEAF_TOKENS, KEY_VALUE_HEADS * HEAD_SIZE))
    return sampled_values.astype(jnp.bfloat16)


def draw_parents(key, part):
    branch_ids = jnp.arange(BRANCHES, dtype=jnp.int32)
    raw_draw = jax.random.randint(jax.random.fold_in(key, 16), (SEARCH_TREES, BRANCHES), 0, 4 * BRANCHES, dtype=jnp.int32)
    return (raw_draw % (branch_ids[None, :] + 1)).astype(jnp.int32)


def place_ends(values, rng, smallest, high):
    longest = values.shape.index(max(values.shape))
    spots = []
    for shift in (0, 1):
        where = [jax.random.randint(jax.random.fold_in(rng, axis), (), 0, length) for axis, length in enumerate(values.shape)]
        where[longest] = (where[longest] + shift) % values.shape[longest]
        spots.append(tuple(where))
    return values.at[spots[0]].set(smallest).at[spots[1]].set(high)


def levels(key, shape, pieces, smallest, largest):
    factor_of = 1.0
    for dim, shards_of in pieces:
        heights = jax.random.uniform(jax.random.fold_in(jax.random.fold_in(key, 6), dim), (shards_of,), jnp.float32, smallest / len(pieces), largest / len(pieces))
        factor_of = factor_of * jnp.repeat(jnp.exp(heights), shape[dim] // shards_of).reshape((-1,) + (1,) * (len(shape) - 1 - dim))
    return factor_of


def split_up(count, total, bound, slope):
    weights = [(1 << 20) // math.isqrt(rank ** slope) + 1 for rank in range(2, count + 1)]
    surplus, given = total - bound - (count - 1), [1] * (count - 1)
    while surplus > 0:
        candidates = [i for i in range(count - 1) if given[i] < bound]
        whole, left = sum([weights[i] for i in candidates]), surplus
        for i in candidates:
            extra = min(bound - given[i], max(1, left * weights[i] // whole), surplus)
            given[i] = given[i] + extra
            surplus = surplus - extra
    return np.array([bound] + given)


def ragged_sizes(own_key, amount, total, reach, skew):
    if amount == 2:
        one = jax.random.randint(own_key, (), max(1, total - reach), min(reach, total - 1) + 1)
        return jnp.stack([one, total - one])
    sizes = jnp.asarray(split_up(amount, total, reach, skew), jnp.int32)
    couples = (amount - 1) // 2
    giver, sink = sizes[1:1 + 2 * couples:2], sizes[2:2 + 2 * couples:2]
    margin = jnp.minimum(giver - 1, reach - sink)
    passed = jax.random.randint(jax.random.fold_in(own_key, 1), (couples,), 0, 1 << 20) % (margin + 1)
    sizes = sizes.at[1:1 + 2 * couples:2].set(giver - passed).at[2:2 + 2 * couples:2].set(sink + passed)
    return sizes[jax.random.permutation(jax.random.fold_in(own_key, 2), amount)]


def normal_values(own_key, dims, width, bound, cuts=(), kind=jnp.bfloat16):
    values = width * jax.random.normal(own_key, dims, jnp.float32)
    if cuts:
        values = values * levels(own_key, dims, cuts, -0.22, 0.18)
    return jnp.clip(values, -bound, bound).astype(kind)


def setup_inputs(seed: int = 0) -> dict:
    keys = jax.random.split(jax.random.key(seed), 13)
    return {
        "prompt_q": draw_prompt_q(jax.random.fold_in(keys[12], 71), 0),
        "prompt_k": draw_prompt_k(jax.random.fold_in(keys[12], 71), 0),
        "prompt_value_rows": normal_values(keys[2], (SEARCH_TREES, PROMPT_TOKENS, KEY_VALUE_HEADS * HEAD_SIZE), 1.0, 6.0, ((0, 16), (1, 8))),
        "leaf_q": draw_leaf_q(jax.random.fold_in(keys[12], 71), 0),
        "leaf_k": draw_leaf_k(jax.random.fold_in(keys[12], 71), 0),
        "leaf_value_rows": normal_values(keys[5], (SEARCH_TREES, LEAF_TOKENS, KEY_VALUE_HEADS * HEAD_SIZE), 1.0, 6.0, ((0, 16), (1, 8))),
        "prompt_dy": normal_values(keys[6], (SEARCH_TREES, PROMPT_TOKENS, D), 1.0, 6.0, ((0, 16), (1, 8))),
        "leaf_dy": normal_values(keys[7], (SEARCH_TREES, LEAF_TOKENS, D), 1.0, 6.0, ((0, 16), (1, 8))),
        "out_weight": normal_values(keys[8], (QUERY_HEADS * HEAD_SIZE, D), (QUERY_HEADS * HEAD_SIZE) ** -0.5, 0.125),
        "lengths": jax.vmap(lambda own: ragged_sizes(own, BRANCHES, LEAF_TOKENS, MOSTLEN, 2))(jax.random.split(keys[9], SEARCH_TREES)).reshape((SEARCH_TREES, BRANCHES)).astype(jnp.int32),
        "offsets": place_ends(jax.random.randint(keys[10], (SEARCH_TREES, BRANCHES), 1, PROMPT_TOKENS + 1), jax.random.fold_in(keys[10], 1), 1, PROMPT_TOKENS).astype(jnp.int32),
        "parents": draw_parents(jax.random.fold_in(keys[12], 71), 0),
    }


def leaf_visibility(lengths, offsets, parents, query_index, prompt_total, leaf_total):
    branch_ends = jnp.cumsum(lengths).astype(jnp.int32)
    branch_ids = jnp.arange(lengths.shape[0], dtype=jnp.int32)
    leaf_index = jnp.arange(leaf_total, dtype=jnp.int32)
    key_branch = lax.optimization_barrier(jnp.sum((leaf_index[:, None] >= branch_ends[None, :]).astype(jnp.int32), axis=1))
    query_branch = lax.optimization_barrier(jnp.sum((query_index[:, None] >= branch_ends[None, :]).astype(jnp.int32), axis=1))
    member = (query_branch[:, None] == branch_ids[None, :]).astype(jnp.int32)
    fork_point = lax.optimization_barrier(jnp.sum(member * offsets[None, :], axis=1))
    ancestor = lax.optimization_barrier(jnp.sum(member * parents[None, :], axis=1))
    prompt_index = jnp.arange(prompt_total, dtype=jnp.int32)
    sees_prompt = prompt_index[None, :] < fork_point[:, None]
    own_branch = (key_branch[None, :] == query_branch[:, None]) & (leaf_index[None, :] <= query_index[:, None])
    inherited = (key_branch[None, :] == ancestor[:, None]) & (ancestor[:, None] != query_branch[:, None])
    return jnp.concatenate([sees_prompt, own_branch | inherited], axis=1)

def tree_pass(query_rows, key_rows, value_rows, upstream, out_weight, visible):
    count_of_rows = query_rows.shape[0]
    score_scale = 1.0 / math.sqrt(HEAD_SIZE)
    grouped_queries = query_rows.reshape(count_of_rows, KEY_VALUE_HEADS, QUERY_PER_KV, HEAD_SIZE).astype(jnp.float32)
    output_gradient = jnp.dot(upstream, out_weight.T, preferred_element_type=jnp.float32).astype(jnp.bfloat16)
    gradient_groups = output_gradient.reshape(count_of_rows, KEY_VALUE_HEADS, QUERY_PER_KV, HEAD_SIZE).astype(jnp.float32)
    attn_parts, dq_parts, dk_parts, dv_parts = ([], [], [], [])
    for key_value_group in range(KEY_VALUE_HEADS):
        key_block = key_rows[:, key_value_group * HEAD_SIZE:(key_value_group + 1) * HEAD_SIZE].astype(jnp.float32)
        value_block = value_rows[:, key_value_group * HEAD_SIZE:(key_value_group + 1) * HEAD_SIZE].astype(jnp.float32)
        scores = jnp.einsum('qhd,kd->hqk', grouped_queries[:, key_value_group], key_block) * score_scale
        scores = jnp.where(visible[None], scores, -jnp.inf)
        shifted = jnp.exp(scores - lax.optimization_barrier(jnp.max(scores, axis=2, keepdims=True)))
        probabilities = shifted / lax.optimization_barrier(jnp.sum(shifted, axis=2, keepdims=True))
        weights = probabilities.astype(jnp.bfloat16).astype(jnp.float32)
        attn_block = jnp.einsum('hqk,kd->qhd', weights, value_block).astype(jnp.bfloat16)
        row_dot = lax.optimization_barrier(jnp.sum(gradient_groups[:, key_value_group] * attn_block.astype(jnp.float32), axis=2))
        prob_grad = jnp.einsum('qhd,kd->hqk', gradient_groups[:, key_value_group], value_block)
        dscore = (probabilities * (prob_grad - row_dot.T[:, :, None]) * score_scale).astype(jnp.bfloat16).astype(jnp.float32)
        dq_parts.append(jnp.einsum('hqk,kd->qhd', dscore, key_block))
        dk_parts.append(jnp.einsum('hqk,qhd->kd', dscore, grouped_queries[:, key_value_group]))
        dv_parts.append(jnp.einsum('hqk,qhd->kd', weights, gradient_groups[:, key_value_group]))
        attn_parts.append(attn_block)
    attn_out = jnp.stack(attn_parts, axis=1).reshape(count_of_rows, QUERY_HEADS * HEAD_SIZE)
    query_grad = jnp.stack(dq_parts, axis=1).reshape(count_of_rows, QUERY_HEADS * HEAD_SIZE)
    return (attn_out, query_grad, jnp.concatenate(dk_parts, axis=1), jnp.concatenate(dv_parts, axis=1))

def reference(prompt_q, prompt_k, prompt_value_rows, leaf_q, leaf_k, leaf_value_rows, prompt_dy, leaf_dy, out_weight, lengths, offsets, parents):
    prompt_index = jnp.arange(PROMPT_TOKENS, dtype=jnp.int32)
    prompt_sees = jnp.concatenate([prompt_index[None, :] <= prompt_index[:, None], jnp.zeros((PROMPT_TOKENS, LEAF_TOKENS), dtype=jnp.bool_)], axis=1)
    leaf_index = jnp.arange(LEAF_TOKENS, dtype=jnp.int32)

    def one_tree(tree_index):
        query_rows = jnp.concatenate([prompt_q[tree_index], leaf_q[tree_index]], axis=0)
        key_rows = jnp.concatenate([prompt_k[tree_index], leaf_k[tree_index]], axis=0)
        value_rows = jnp.concatenate([prompt_value_rows[tree_index], leaf_value_rows[tree_index]], axis=0)
        upstream = jnp.concatenate([prompt_dy[tree_index], leaf_dy[tree_index]], axis=0)
        leaf_sees = leaf_visibility(lengths[tree_index], offsets[tree_index], parents[tree_index], leaf_index, PROMPT_TOKENS, LEAF_TOKENS)
        visible = jnp.concatenate([prompt_sees, leaf_sees], axis=0)
        return tree_pass(query_rows, key_rows, value_rows, upstream, out_weight, visible)
    attn_out, query_grad, key_grad, value_grad = lax.map(one_tree, jnp.arange(SEARCH_TREES, dtype=jnp.int32))
    upstream_all = jnp.concatenate([prompt_dy, leaf_dy], axis=1)
    summed = jnp.dot(attn_out.reshape(-1, QUERY_HEADS * HEAD_SIZE).T, upstream_all.reshape(-1, D), preferred_element_type=jnp.float32)
    weight_grad = summed * (1.0 / math.sqrt(SEARCH_TREES * (PROMPT_TOKENS + LEAF_TOKENS)))
    return (query_grad[:, :PROMPT_TOKENS], key_grad[:, :PROMPT_TOKENS], value_grad[:, :PROMPT_TOKENS], query_grad[:, PROMPT_TOKENS:], key_grad[:, PROMPT_TOKENS:], value_grad[:, PROMPT_TOKENS:], weight_grad)
```

```python
import functools
import math

import jax
import jax.numpy as jnp
import numpy as np
from jax import lax
from jax.experimental import pallas as pl
from jax.experimental.pallas import tpu as pltpu
from jax.sharding import PartitionSpec as P

MESH = pl.DeviceIdType.MESH
HEAD = 128
HEADS = 14
GROUPS = 2
PER_KV = 7
WIDTH = HEADS * HEAD
D = 3584
PROMPT = 128
LEAF = 48
ROWS = PROMPT + LEAF
PEERS = 8
KEYS = PEERS * ROWS
TOKENS = 16 * KEYS
SHARE = 14
CHUNK = 16 * SHARE
SCALE = 1.0 / math.sqrt(HEAD)
LOG2E = 1.0 / math.log(2.0)
NEG = -1e30
PARTS = ((0, 1536), (1536, 1024), (2560, 1024))
VMEM = pltpu.MemorySpace.VMEM
LIMIT = 60 * 1024 * 1024
F32 = jnp.float32
BF16 = jnp.bfloat16


def nt(a, b):
    return lax.dot_general(a, b, (((1,), (1,)), ((), ())), preferred_element_type=F32)


def nn(a, b):
    return lax.dot_general(a, b, (((1,), (0,)), ((), ())), preferred_element_type=F32)


def tn(a, b):
    return lax.dot_general(a, b, (((0,), (0,)), ((), ())), preferred_element_type=F32)


def send_to(src, dst, send_sem, recv_sem, device):
    return pltpu.make_async_remote_copy(
        src_ref=src,
        dst_ref=dst,
        send_sem=send_sem,
        recv_sem=recv_sem,
        device_id=device,
        device_id_type=MESH,
    )


def flip(value, bit):
    low = (value // bit) % 2
    return value + bit - 2 * bit * low


def seq_peers(seq):
    found = []
    for d in range(1, PEERS):
        p = seq
        for bit in (1, 2, 4):
            if d & bit:
                p = flip(p, bit)
        found.append(p)
    return found


def gather_kernel(
    pk, pv, lk, lv, pdy, ldy, w, kv, g, yp, dy, wbuf,
    lsem, dsem, wsem, ssem, rsem, ysend, yrecv,
):
    leaf = lax.axis_index("leaf")
    seq = lax.axis_index("seq")
    twin = (flip(leaf, 1), seq)
    peers = seq_peers(seq)
    mine = [
        pltpu.make_async_copy(pk, kv.at[seq, 0:PROMPT, 0:256], lsem.at[0]),
        pltpu.make_async_copy(pv, kv.at[seq, 0:PROMPT, 256:512], lsem.at[1]),
        pltpu.make_async_copy(lk, kv.at[seq, PROMPT:ROWS, 0:256], lsem.at[2]),
        pltpu.make_async_copy(lv, kv.at[seq, PROMPT:ROWS, 256:512], lsem.at[3]),
    ]
    for c in mine:
        c.start()
    ups = [
        pltpu.make_async_copy(pdy, dy.at[0:PROMPT], dsem.at[0]),
        pltpu.make_async_copy(ldy, dy.at[PROMPT:ROWS], dsem.at[1]),
    ]
    for c in ups:
        c.start()
    tiles = WIDTH // 256
    for t in range(tiles):
        pltpu.make_async_copy(w.at[t * 256:(t + 1) * 256], wbuf.at[t], wsem.at[t]).start()
    barrier = pltpu.get_barrier_semaphore()
    for p in peers:
        pl.semaphore_signal(barrier, inc=1, device_id=(leaf, p), device_id_type=MESH)
    pl.semaphore_signal(barrier, inc=1, device_id=twin, device_id_type=MESH)
    pl.semaphore_wait(barrier, PEERS)
    for c in mine:
        c.wait()
    out = []
    for i, p in enumerate(peers):
        c = send_to(kv.at[seq], kv.at[seq], ssem.at[i], rsem.at[i], (leaf, p))
        c.start()
        out.append(c)
    ys = [
        send_to(pdy, yp.at[0:PROMPT], ysend.at[0], yrecv.at[0], twin),
        send_to(ldy, yp.at[PROMPT:ROWS], ysend.at[1], yrecv.at[1], twin),
    ]
    for c in ys:
        c.start()
    for c in ups:
        c.wait()

    def tile(t, carry):
        pltpu.make_async_copy(w.at[0:256], wbuf.at[t], wsem.at[t]).wait()
        acc = nt(dy[...], wbuf[t]).astype(BF16)
        g[2 * t] = acc[:, 0:HEAD]
        g[2 * t + 1] = acc[:, HEAD:256]
        return carry

    lax.fori_loop(0, tiles, tile, 0)
    for i, p in enumerate(peers):
        send_to(kv.at[p], kv.at[p], ssem.at[i], rsem.at[i], (leaf, p)).wait_recv()
    for c in out:
        c.wait_send()
    for c in ys:
        c.wait()


def gather_call(pk, pv, lk, lv, pdy, ldy, w):
    any_ = pl.BlockSpec(memory_space=pl.ANY)
    vm = pl.BlockSpec(memory_space=VMEM)
    return pl.pallas_call(
        gather_kernel,
        out_shape=(
            jax.ShapeDtypeStruct((PEERS, ROWS, 512), BF16),
            jax.ShapeDtypeStruct((HEADS, ROWS, HEAD), BF16),
            jax.ShapeDtypeStruct((ROWS, D), BF16),
        ),
        in_specs=[any_] * 7,
        out_specs=(vm, vm, any_),
        scratch_shapes=[
            pltpu.VMEM((ROWS, D), BF16),
            pltpu.VMEM((WIDTH // 256, 256, D), BF16),
            pltpu.SemaphoreType.DMA((4,)),
            pltpu.SemaphoreType.DMA((2,)),
            pltpu.SemaphoreType.DMA((WIDTH // 256,)),
            pltpu.SemaphoreType.DMA((PEERS - 1,)),
            pltpu.SemaphoreType.DMA((PEERS - 1,)),
            pltpu.SemaphoreType.DMA((2,)),
            pltpu.SemaphoreType.DMA((2,)),
        ],
        compiler_params=pltpu.CompilerParams(
            collective_id=0, has_side_effects=True, vmem_limit_bytes=LIMIT
        ),
        name="gather",
    )(pk, pv, lk, lv, pdy, ldy, w)


def attention_kernel(
    pq, lq, kv, g, bias, dqp, dql, atp, dkv, qs, ws, ds, at, perm
):
    for h in range(HEADS):
        cols = slice(h * HEAD, (h + 1) * HEAD)
        qs[h, 0:PROMPT, :] = pq[:, cols]
        qs[h, PROMPT:ROWS, :] = lq[:, cols]
    for grp in range(GROUPS):
        key = kv[:, grp * HEAD:(grp + 1) * HEAD]
        value = kv[:, 256 + grp * HEAD:256 + (grp + 1) * HEAD]

        def head(j, carry):
            h = grp * PER_KV + j
            q = qs[h]
            gh = g[h]
            s = nt(q, key) * (SCALE * LOG2E) + bias[...]
            top = jnp.max(s, axis=1, keepdims=True)
            e = jnp.exp2(s - top)
            total = jnp.sum(e, axis=1, keepdims=True)
            prob = e / total
            weight = prob.astype(BF16)
            ws[j] = weight
            a = nn(weight, value).astype(BF16).astype(F32)
            at[pl.ds(pl.multiple_of(h * HEAD, HEAD), HEAD), :] = a.T
            dot = jnp.sum(gh.astype(F32) * a, axis=1, keepdims=True)
            dp = nt(gh, value)
            dsc = (prob * ((dp - dot) * SCALE)).astype(BF16)
            ds[j] = dsc
            dq = nn(dsc, key)
            cols = pl.ds(pl.multiple_of(h * HEAD, HEAD), HEAD)
            dqp[:, cols] = dq[0:PROMPT]
            dql[:, cols] = dq[PROMPT:ROWS]
            return carry

        lax.fori_loop(0, PER_KV, head, 0)
        stack = slice(grp * PER_KV, (grp + 1) * PER_KV)
        tall = PER_KV * ROWS
        dk = tn(qs[stack].reshape(tall, HEAD), ds[...].reshape(tall, KEYS))
        dkv[:, grp * HEAD:(grp + 1) * HEAD] = dk.T.astype(BF16)
        dv = tn(g[stack].reshape(tall, HEAD), ws[...].reshape(tall, KEYS))
        dkv[:, 256 + grp * HEAD:256 + (grp + 1) * HEAD] = dv.T.astype(BF16)
    for c in range(2):
        for y in range(4):
            for zh in range(2):
                n = y * 448 + zh * 224 + c * 112
                atp[0, c, y, zh * 112:(zh + 1) * 112, :] = at[n:n + 112, :].astype(BF16)
        for x in range(4):
            for y in range(4):
                for z in range(4):
                    n = y * 448 + (z // 2) * 224 + c * 112 + (z % 2) * 56 + x * SHARE
                    r = x * CHUNK + y * 56 + z * SHARE
                    perm[0, r:r + SHARE, :] = at[n:n + SHARE, :]
                    r = z * CHUNK + x * 56 + y * SHARE
                    perm[1, r:r + SHARE, :] = at[n:n + SHARE, :]
        for k in range(4):
            atp[1, c, k] = perm[0, k * CHUNK:(k + 1) * CHUNK, :].astype(BF16)
            atp[2, c, k] = perm[1, k * CHUNK:(k + 1) * CHUNK, :].astype(BF16)


def attention_call(pq, lq, kv, g, bias):
    vm = pl.BlockSpec(memory_space=VMEM)
    return pl.pallas_call(
        attention_kernel,
        out_shape=(
            jax.ShapeDtypeStruct((PROMPT, WIDTH), F32),
            jax.ShapeDtypeStruct((LEAF, WIDTH), F32),
            jax.ShapeDtypeStruct((3, 2, 4, CHUNK, ROWS), BF16),
            jax.ShapeDtypeStruct((KEYS, 512), BF16),
        ),
        in_specs=[vm] * 5,
        out_specs=(vm,) * 4,
        scratch_shapes=[
            pltpu.VMEM((HEADS, ROWS, HEAD), BF16),
            pltpu.VMEM((PER_KV, ROWS, KEYS), BF16),
            pltpu.VMEM((PER_KV, ROWS, KEYS), BF16),
            pltpu.VMEM((WIDTH, ROWS), F32),
            pltpu.VMEM((2, 4 * CHUNK, ROWS), F32),
        ],
        compiler_params=pltpu.CompilerParams(vmem_limit_bytes=LIMIT),
        name="attention",
    )(pq, lq, kv, g, bias)


def reduce_kernel(
    atp, pdy, ldy, yp, dkv, wg, dk, dv, *scratch
):
    (yo, yt, ap) = scratch[0:3]
    pb = scratch[3:6]
    own = scratch[6:9]
    rel = scratch[9:12]
    rin = scratch[12:15]
    b2 = scratch[15:18]
    r2 = scratch[18:21]
    b3 = scratch[21:24]
    r3 = scratch[24:27]
    (kin, lsem, asend, arecv, ksend, krecv, s1, v1, s2, v2, s3, v3) = scratch[27:]
    leaf = lax.axis_index("leaf")
    seq = lax.axis_index("seq")
    core = leaf % 2
    y = leaf // 4
    z = ((leaf // 2) % 2) * 2 + seq // 4
    x = seq % 4
    twin = (flip(leaf, 1), seq)
    peers = seq_peers(seq)

    def on_x(k):
        return (leaf, (seq // 4) * 4 + (x + k) % 4)

    def on_y(k):
        return (((y + k) % 4) * 4 + leaf % 4, seq)

    def on_z(k):
        other = (z + k) % 4
        return (y * 4 + (other // 2) * 2 + core, (other % 2) * 4 + x)

    axes = ((on_y, on_z, on_x), (on_x, on_y, on_z), (on_z, on_x, on_y))
    spots = ((y, z, x), (x, y, z), (z, x, y))

    loads = [
        pltpu.make_async_copy(pdy, yo.at[0:PROMPT], lsem.at[0]),
        pltpu.make_async_copy(ldy, yo.at[PROMPT:ROWS], lsem.at[1]),
        pltpu.make_async_copy(yp, yt, lsem.at[2]),
    ]
    for c in loads:
        c.start()
    barrier = pltpu.get_barrier_semaphore()
    greet = [(leaf, p) for p in peers] + [twin]
    greet += [on_y(k) for k in (1, 2, 3)] + [on_z(k) for k in (1, 2, 3)]
    for d in greet:
        pl.semaphore_signal(barrier, inc=1, device_id=d, device_id_type=MESH)
    pl.semaphore_wait(barrier, len(greet))

    swaps = []
    for p in range(3):
        c = send_to(atp.at[p, 1 - core], ap.at[p], asend.at[p], arecv.at[p], twin)
        c.start()
        swaps.append(c)
    for c in loads:
        c.wait()
    for c in swaps:
        c.wait_recv()

    started = []

    def go(src, dst, send_sem, recv_sem, device):
        c = send_to(src, dst, send_sem, recv_sem, device)
        c.start()
        started.append(c)
        return c

    def product(p, k):
        first, wide = PARTS[p]
        dest = (spots[p][0] + k) % 4
        cols = slice(first, first + wide)
        return nn(atp[p, core, dest], yo[:, cols]) + nn(ap[p, dest], yt[:, cols])

    relays = {}
    direct = {}
    for p in range(3):
        h = PARTS[p][1] // 2
        pb[p][2] = product(p, 2).astype(BF16)
        relays[p, 0] = go(pb[p].at[2, :, 0:h], rel[p].at[0], s1.at[p, 0], v1.at[p, 0], axes[p][0](1))
        relays[p, 1] = go(pb[p].at[2, :, h:2 * h], rel[p].at[1], s1.at[p, 1], v1.at[p, 1], axes[p][0](3))
    for p in range(3):
        h = PARTS[p][1] // 2
        pb[p][1] = product(p, 1).astype(BF16)
        direct[p, 0] = go(pb[p].at[1, :, h:2 * h], rin[p].at[0, :, h:2 * h], s1.at[p, 2], v1.at[p, 2], axes[p][0](1))
        pb[p][3] = product(p, 3).astype(BF16)
        direct[p, 1] = go(pb[p].at[3, :, 0:h], rin[p].at[1, :, 0:h], s1.at[p, 3], v1.at[p, 3], axes[p][0](3))
    for p in range(3):
        own[p][...] = product(p, 0)
    for p in (1, 2, 0):
        h = PARTS[p][1] // 2
        relays[p, 0].wait_recv()
        pb[p][1, :, 0:h] = (pb[p][1, :, 0:h].astype(F32) + rel[p][0].astype(F32)).astype(BF16)
        direct[p, 2] = go(pb[p].at[1, :, 0:h], rin[p].at[0, :, 0:h], s1.at[p, 4], v1.at[p, 4], axes[p][0](1))
        relays[p, 1].wait_recv()
        pb[p][3, :, h:2 * h] = (pb[p][3, :, h:2 * h].astype(F32) + rel[p][1].astype(F32)).astype(BF16)
        direct[p, 3] = go(pb[p].at[3, :, h:2 * h], rin[p].at[1, :, h:2 * h], s1.at[p, 5], v1.at[p, 5], axes[p][0](3))
    grads = []
    for i, q in enumerate(peers):
        grads.append(go(dkv.at[q], kin.at[i], ksend.at[i], krecv.at[i], (leaf, q)))
    second = {}
    for p in (1, 2, 0):
        wide = PARTS[p][1]
        for i in range(4):
            direct[p, i].wait_recv()
        pad = jnp.zeros((8, wide), F32)
        for j in range(4):
            rows = slice(j * 56, (j + 1) * 56)
            full = own[p][rows] + rin[p][0, rows].astype(F32) + rin[p][1, rows].astype(F32)
            b2[p][j] = jnp.concatenate([full, pad], axis=0).astype(BF16)
        spot = spots[p][1]
        for k in (2, 1, 3):
            second[p, k] = go(b2[p].at[(spot + k) % 4], r2[p].at[k - 1], s2.at[p, k - 1], v2.at[p, k - 1], axes[p][1](k))
    third = {}
    for p in (1, 2, 0):
        for k in (1, 2, 3):
            second[p, k].wait_recv()
        full = b2[p][spots[p][1]].astype(F32)
        for k in range(3):
            full = full + r2[p][k].astype(F32)
        pad = jnp.zeros((2, PARTS[p][1]), F32)
        for j in range(4):
            piece = full[j * SHARE:(j + 1) * SHARE]
            b3[p][j] = jnp.concatenate([piece, pad], axis=0).astype(BF16)
        spot = spots[p][2]
        for k in (2, 1, 3):
            third[p, k] = go(b3[p].at[(spot + k) % 4], r3[p].at[k - 1], s3.at[p, k - 1], v3.at[p, k - 1], axes[p][2](k))
    for c in grads:
        c.wait_recv()
    block = dkv[seq].astype(F32)
    for i in range(PEERS - 1):
        block = block + kin[i].astype(F32)
    dk[...] = block[:, 0:256]
    dv[...] = block[:, 256:512]
    for p in (1, 2, 0):
        first, wide = PARTS[p]
        for k in (1, 2, 3):
            third[p, k].wait_recv()
        full = b3[p][spots[p][2]].astype(F32)
        for k in range(3):
            full = full + r3[p][k].astype(F32)
        wg[:, first:first + wide] = full[0:SHARE] * (1.0 / math.sqrt(TOKENS))
    for c in swaps:
        c.wait_send()
    for c in started:
        c.wait_send()


def reduce_call(atp, pdy, ldy, yp, dkv):
    any_ = pl.BlockSpec(memory_space=pl.ANY)
    vm = pl.BlockSpec(memory_space=VMEM)
    widths = [w for _, w in PARTS]
    dma = pltpu.SemaphoreType.DMA
    scratch = [
        pltpu.VMEM((ROWS, D), BF16),
        pltpu.VMEM((ROWS, D), BF16),
        pltpu.VMEM((3, 4, CHUNK, ROWS), BF16),
    ]
    scratch += [pltpu.VMEM((4, CHUNK, w), BF16) for w in widths]
    scratch += [pltpu.VMEM((CHUNK, w), F32) for w in widths]
    scratch += [pltpu.VMEM((2, CHUNK, w // 2), BF16) for w in widths]
    scratch += [pltpu.VMEM((2, CHUNK, w), BF16) for w in widths]
    scratch += [pltpu.VMEM((4, 64, w), BF16) for w in widths]
    scratch += [pltpu.VMEM((3, 64, w), BF16) for w in widths]
    scratch += [pltpu.VMEM((4, 16, w), BF16) for w in widths]
    scratch += [pltpu.VMEM((3, 16, w), BF16) for w in widths]
    scratch += [pltpu.VMEM((PEERS - 1, ROWS, 512), BF16), dma((3,)), dma((3,)), dma((3,))]
    scratch += [dma((PEERS - 1,)), dma((PEERS - 1,)), dma((3, 6)), dma((3, 6))]
    scratch += [dma((3, 3)), dma((3, 3)), dma((3, 3)), dma((3, 3))]
    return pl.pallas_call(
        reduce_kernel,
        out_shape=(
            jax.ShapeDtypeStruct((SHARE, D), F32),
            jax.ShapeDtypeStruct((ROWS, 256), F32),
            jax.ShapeDtypeStruct((ROWS, 256), F32),
        ),
        in_specs=[vm, any_, any_, any_, vm],
        out_specs=(vm, vm, vm),
        scratch_shapes=scratch,
        compiler_params=pltpu.CompilerParams(
            collective_id=1, has_side_effects=True, vmem_limit_bytes=LIMIT
        ),
        name="reduce",
    )(atp, pdy, ldy, yp, dkv)


def visibility_bias(lengths, offsets, parents):
    seq = lax.axis_index("seq")
    slot, row = np.divmod(np.arange(KEYS), ROWS)
    key_is_prompt = jnp.asarray(row < PROMPT)
    key_index = jnp.asarray(np.where(row < PROMPT, slot * PROMPT + row, slot * LEAF + row - PROMPT), jnp.int32)
    ends = jnp.cumsum(lengths)
    ids = jnp.arange(lengths.shape[0], dtype=jnp.int32)
    query_leaf = seq * LEAF + jnp.arange(LEAF, dtype=jnp.int32)
    query_prompt = seq * PROMPT + jnp.arange(PROMPT, dtype=jnp.int32)
    key_branch = jnp.sum((key_index[:, None] >= ends[None, :]).astype(jnp.int32), axis=1)
    query_branch = jnp.sum((query_leaf[:, None] >= ends[None, :]).astype(jnp.int32), axis=1)
    member = (query_branch[:, None] == ids[None, :]).astype(jnp.int32)
    fork = jnp.sum(member * offsets[None, :], axis=1)
    ancestor = jnp.sum(member * parents[None, :], axis=1)
    prompt_sees = key_is_prompt[None, :] & (key_index[None, :] <= query_prompt[:, None])
    same = (key_branch[None, :] == query_branch[:, None]) & (key_index[None, :] <= query_leaf[:, None])
    inherited = (key_branch[None, :] == ancestor[:, None]) & (ancestor[:, None] != query_branch[:, None])
    leaf_sees = jnp.where(key_is_prompt[None, :], key_index[None, :] < fork[:, None], same | inherited)
    sees = jnp.concatenate([prompt_sees, leaf_sees], axis=0)
    return jnp.where(sees, 0.0, NEG).astype(F32)


def body(pq, pk, pv, lq, lk, lv, pdy, ldy, w, lengths, offsets, parents):
    bias = visibility_bias(lengths[0], offsets[0], parents[0])
    kv, g, yp = gather_call(pk[0], pv[0], lk[0], lv[0], pdy[0], ldy[0], w)
    dqp, dql, atp, dkv = attention_call(pq[0], lq[0], kv.reshape(KEYS, 512), g, bias)
    wg, dk, dv = reduce_call(atp, pdy[0], ldy[0], yp, dkv.reshape(PEERS, ROWS, 512))
    return (
        dqp[None], dk[None, :PROMPT], dv[None, :PROMPT],
        dql[None], dk[None, PROMPT:], dv[None, PROMPT:], wg,
    )


def solution(mesh):
    rows = P("leaf", "seq", None)
    placed = (rows,) * 8 + (P(),) + (P("leaf", None),) * 3
    return jax.shard_map(
        body,
        mesh=mesh,
        in_specs=placed,
        out_specs=(rows,) * 6 + (P(("leaf", "seq"), None),),
        check_vma=False,
    )
```

```python
import math

import jax
import jax.numpy as jnp
from jax import lax
from jax.experimental import pallas as pl
from jax.experimental.pallas import tpu as pltpu
from jax.sharding import PartitionSpec as P

MESH = pl.DeviceIdType.MESH
HEAD = 128
HEADS = 14
GROUPS = 2
PER_KV = 7
WIDTH = HEADS * HEAD
D = 3584
PROMPT = 128
LEAF = 48
ROWS = PROMPT + LEAF
PEERS = 8
KEYS = PEERS * ROWS
TOKENS = 16 * KEYS
SHARE = 14
BRANCHES = 16
CHUNK = 16 * SHARE
SCALE = 1.0 / math.sqrt(HEAD)
LOG2E = 1.0 / math.log(2.0)
NEG = -1e30
PARTS = ((0, 1536), (1536, 1024), (2560, 1024))
VMEM = pltpu.MemorySpace.VMEM
SMEM = pltpu.MemorySpace.SMEM
HALF = 256
LIMIT = 63 * 1024 * 1024
F32 = jnp.float32
BF16 = jnp.bfloat16


def nt(a, b):
    return lax.dot_general(a, b, (((1,), (1,)), ((), ())), preferred_element_type=F32)


def nn(a, b):
    return lax.dot_general(a, b, (((1,), (0,)), ((), ())), preferred_element_type=F32)


def tn(a, b):
    return lax.dot_general(a, b, (((0,), (0,)), ((), ())), preferred_element_type=F32)


def send_to(src, dst, send_sem, recv_sem, device):
    return pltpu.make_async_remote_copy(
        src_ref=src,
        dst_ref=dst,
        send_sem=send_sem,
        recv_sem=recv_sem,
        device_id=device,
        device_id_type=MESH,
    )


def flip(value, bit):
    low = (value // bit) % 2
    return value + bit - 2 * bit * low


def seq_peers(seq):
    found = []
    for d in range(1, PEERS):
        p = seq
        for bit in (1, 2, 4):
            if d & bit:
                p = flip(p, bit)
        found.append(p)
    return found


def visibility(lengths, offsets, parents, seq, bias):
    rows = lax.broadcasted_iota(jnp.int32, (ROWS, 1), 0)
    is_leaf = rows >= PROMPT
    query = jnp.where(is_leaf, seq * LEAF + rows - PROMPT, seq * PROMPT + rows)
    cols = lax.broadcasted_iota(jnp.int32, (1, KEYS), 1)
    slot = jnp.zeros((1, KEYS), jnp.int32)
    for s in range(1, PEERS):
        slot = slot + (cols >= s * ROWS).astype(jnp.int32)
    spot = cols - slot * ROWS
    key_leaf = spot >= PROMPT
    key = jnp.where(key_leaf, slot * LEAF + spot - PROMPT, slot * PROMPT + spot)
    key_branch = jnp.zeros((1, KEYS), jnp.int32)
    query_branch = jnp.zeros((ROWS, 1), jnp.int32)
    end = jnp.int32(0)
    for b in range(BRANCHES):
        end = end + lengths[0, b]
        key_branch = key_branch + (key >= end).astype(jnp.int32)
        query_branch = query_branch + (query >= end).astype(jnp.int32)
    fork = jnp.zeros((ROWS, 1), jnp.int32)
    ancestor = jnp.zeros((ROWS, 1), jnp.int32)
    for b in range(BRANCHES):
        here = query_branch == b
        fork = jnp.where(here, offsets[0, b], fork)
        ancestor = jnp.where(here, parents[0, b], ancestor)
    ancestor = jnp.where(is_leaf & (ancestor != query_branch), ancestor, -1)
    branch = jnp.where(is_leaf, query_branch, -1)
    reach = jnp.where(is_leaf, fork, query + 1)
    prompt_key = jnp.where(key_leaf, 1 << 20, key)
    key_branch = jnp.where(key_leaf, key_branch, -2)
    sees = prompt_key < reach
    sees = sees | ((key_branch == branch) & (key <= query))
    sees = sees | (key_branch == ancestor)
    bias[...] = jnp.where(sees, 0.0, NEG)


def tree_kernel(
    pq, pk, pv, lq, lk, lv, pdy, ldy, w, lengths, offsets, parents,
    dqp, dql, wg, dkv_out, *scratch
):
    (kv, yo, yt, wbuf, g, qs, attn, ws, ds, at, perm, atp, ap, bias, dkv, kin) = scratch[0:16]
    own = scratch[16:19]
    rel = scratch[19:22]
    rin = scratch[22:25]
    b2 = scratch[25:28]
    r2 = scratch[28:31]
    b3 = scratch[31:34]
    r3 = scratch[34:37]
    (lsem, dsem, wsem, qsem, gsend, grecv, ysend, yrecv, asend, arecv,
     ksend, krecv, s1, v1, s2, v2, s3, v3) = scratch[37:]
    leaf = lax.axis_index("leaf")
    seq = lax.axis_index("seq")
    core = leaf % 2
    y = leaf // 4
    plane = seq // 4
    z = ((leaf // 2) % 2) * 2 + plane
    x = seq % 4
    twin = (flip(leaf, 1), seq)
    peers = seq_peers(seq)

    def slot(q, k):
        return q * 4 + (x + k) % 4

    def on_x(k):
        return (leaf, slot(plane, k))

    def on_y(k):
        return (((y + k) % 4) * 4 + leaf % 4, seq)

    def on_z(k):
        other = (z + k) % 4
        return (y * 4 + (other // 2) * 2 + core, (other % 2) * 4 + x)

    across = (leaf, slot(1 - plane, 0))
    axes = ((on_y, on_z, on_x), (on_x, on_y, on_z), (on_z, on_x, on_y))
    spots = ((y, z, x), (x, y, z), (z, x, y))

    mine = [
        pltpu.make_async_copy(pk, kv.at[seq, 0:PROMPT, 0:256], lsem.at[0]),
        pltpu.make_async_copy(pv, kv.at[seq, 0:PROMPT, 256:512], lsem.at[1]),
        pltpu.make_async_copy(lk, kv.at[seq, PROMPT:ROWS, 0:256], lsem.at[2]),
        pltpu.make_async_copy(lv, kv.at[seq, PROMPT:ROWS, 256:512], lsem.at[3]),
    ]
    for c in mine:
        c.start()
    ups = [
        pltpu.make_async_copy(pdy, yo.at[0:PROMPT], dsem.at[0]),
        pltpu.make_async_copy(ldy, yo.at[PROMPT:ROWS], dsem.at[1]),
    ]
    for c in ups:
        c.start()
    tiles = WIDTH // 256
    for t in range(tiles):
        pltpu.make_async_copy(w.at[t * 256:(t + 1) * 256], wbuf.at[t], wsem.at[t]).start()
    queries = []
    for h in range(HEADS):
        cols = slice(h * HEAD, (h + 1) * HEAD)
        queries.append(pltpu.make_async_copy(pq.at[:, cols], qs.at[h, 0:PROMPT], qsem.at[h, 0]))
        queries.append(pltpu.make_async_copy(lq.at[:, cols], qs.at[h, PROMPT:ROWS], qsem.at[h, 1]))
    for c in queries:
        c.start()
    barrier = pltpu.get_barrier_semaphore()
    greet = [(leaf, p) for p in peers] + [twin]
    greet += [on_y(k) for k in (1, 2, 3)] + [on_z(k) for k in (1, 2, 3)]
    for d in greet:
        pl.semaphore_signal(barrier, inc=1, device_id=d, device_id_type=MESH)
    pl.semaphore_wait(barrier, len(greet))
    started = []

    def go(src, dst, send_sem, recv_sem, device):
        c = send_to(src, dst, send_sem, recv_sem, device)
        c.start()
        started.append(c)
        return c

    def pass_on(ref, i, device):
        return go(ref, ref, gsend.at[i], grecv.at[i], device)

    def arrived(ref, i):
        send_to(ref, ref, gsend.at[i], grecv.at[i], across).wait_recv()

    for c in mine:
        c.wait()
    block = kv.at[seq]
    pass_on(block, 0, across)
    pass_on(block, 1, on_x(1))
    pass_on(block, 2, on_x(3))
    swaps = [
        go(pdy, yt.at[0:PROMPT], ysend.at[0], yrecv.at[0], twin),
        go(ldy, yt.at[PROMPT:ROWS], ysend.at[1], yrecv.at[1], twin),
    ]
    for c in ups:
        c.wait()

    def tile(t, carry):
        pltpu.make_async_copy(w.at[0:256], wbuf.at[t], wsem.at[t]).wait()
        acc = nt(yo[...], wbuf[t]).astype(BF16)
        g[2 * t] = acc[:, 0:HEAD]
        g[2 * t + 1] = acc[:, HEAD:256]
        return carry

    lax.fori_loop(0, tiles, tile, 0)
    arrived(kv.at[slot(plane, 3)], 1)
    pass_on(kv.at[slot(plane, 3), :, 0:HALF], 3, on_x(1))
    arrived(kv.at[slot(plane, 1)], 2)
    pass_on(kv.at[slot(plane, 1), :, HALF:512], 4, on_x(3))
    arrived(kv.at[slot(1 - plane, 0)], 0)
    pass_on(kv.at[slot(1 - plane, 0)], 5, on_x(1))
    pass_on(kv.at[slot(1 - plane, 0)], 6, on_x(3))
    visibility(lengths, offsets, parents, seq, bias)
    arrived(kv.at[slot(plane, 2), :, 0:HALF], 3)
    arrived(kv.at[slot(plane, 2), :, HALF:512], 4)
    pass_on(kv.at[slot(plane, 2)], 7, across)
    for c in queries:
        c.wait()
    arrived(kv.at[slot(1 - plane, 3)], 5)
    arrived(kv.at[slot(1 - plane, 1)], 6)
    arrived(kv.at[slot(1 - plane, 2)], 7)

    def keys_of(grp):
        cols = pl.ds(pl.multiple_of(grp * HEAD, HEAD), HEAD)
        return kv[:, :, cols].reshape(KEYS, HEAD)

    def values_of(grp):
        cols = pl.ds(pl.multiple_of(256 + grp * HEAD, HEAD), HEAD)
        return kv[:, :, cols].reshape(KEYS, HEAD)

    def forward(h, carry):
        grp = h // PER_KV
        s = nt(qs[h], keys_of(grp)) * (SCALE * LOG2E) + bias[...]
        top = jnp.max(s, axis=1, keepdims=True)
        e = jnp.exp2(s - top)
        total = jnp.sum(e, axis=1, keepdims=True)
        weight = (e / total).astype(BF16)
        ws[h] = weight
        a = nn(weight, values_of(grp)).astype(BF16)
        attn[h] = a
        at[pl.ds(pl.multiple_of(h * HEAD, HEAD), HEAD), :] = a.astype(F32).T
        return carry

    lax.fori_loop(0, HEADS, forward, 0)
    for c in range(2):
        for yy in range(4):
            for zh in range(2):
                n = yy * 448 + zh * 224 + c * 112
                atp[0, c, yy, zh * 112:(zh + 1) * 112, :] = at[n:n + 112, :].astype(BF16)
        for xx in range(4):
            for yy in range(4):
                for zz in range(4):
                    n = yy * 448 + (zz // 2) * 224 + c * 112 + (zz % 2) * 56 + xx * SHARE
                    r = xx * CHUNK + yy * 56 + zz * SHARE
                    perm[0, r:r + SHARE, :] = at[n:n + SHARE, :]
                    r = zz * CHUNK + xx * 56 + yy * SHARE
                    perm[1, r:r + SHARE, :] = at[n:n + SHARE, :]
        for k in range(4):
            atp[1, c, k] = perm[0, k * CHUNK:(k + 1) * CHUNK, :].astype(BF16)
            atp[2, c, k] = perm[1, k * CHUNK:(k + 1) * CHUNK, :].astype(BF16)
    rows = []
    for p in range(3):
        rows.append(go(atp.at[p, 1 - core], ap.at[p], asend.at[p], arecv.at[p], twin))
    for c in swaps:
        c.wait_recv()
    for c in rows:
        c.wait_recv()

    def part(p, k, lo, hi):
        first = PARTS[p][0]
        return wbuf.at[k, 0:CHUNK, first + lo:first + hi]

    def product(p, k):
        first, wide = PARTS[p]
        dest = (spots[p][0] + k) % 4
        cols = slice(first, first + wide)
        return nn(atp[p, core, dest], yo[:, cols]) + nn(ap[p, dest], yt[:, cols])

    relays = {}
    direct = {}
    for p in range(3):
        wide = PARTS[p][1]
        h = wide // 2
        part(p, 2, 0, wide)[...] = product(p, 2).astype(BF16)
        relays[p, 0] = go(part(p, 2, 0, h), rel[p].at[0], s1.at[p, 0], v1.at[p, 0], axes[p][0](1))
        relays[p, 1] = go(part(p, 2, h, wide), rel[p].at[1], s1.at[p, 1], v1.at[p, 1], axes[p][0](3))
    for p in range(3):
        wide = PARTS[p][1]
        h = wide // 2
        part(p, 1, 0, wide)[...] = product(p, 1).astype(BF16)
        direct[p, 0] = go(part(p, 1, h, wide), rin[p].at[0, :, h:wide], s1.at[p, 2], v1.at[p, 2], axes[p][0](1))
        part(p, 3, 0, wide)[...] = product(p, 3).astype(BF16)
        direct[p, 1] = go(part(p, 3, 0, h), rin[p].at[1, :, 0:h], s1.at[p, 3], v1.at[p, 3], axes[p][0](3))
    for p in range(3):
        own[p][...] = product(p, 0)

    def relay(p):
        wide = PARTS[p][1]
        h = wide // 2
        relays[p, 0].wait_recv()
        here = part(p, 1, 0, h)
        here[...] = (here[...].astype(F32) + rel[p][0].astype(F32)).astype(BF16)
        direct[p, 2] = go(here, rin[p].at[0, :, 0:h], s1.at[p, 4], v1.at[p, 4], axes[p][0](1))
        relays[p, 1].wait_recv()
        here = part(p, 3, h, wide)
        here[...] = (here[...].astype(F32) + rel[p][1].astype(F32)).astype(BF16)
        direct[p, 3] = go(here, rin[p].at[1, :, h:wide], s1.at[p, 5], v1.at[p, 5], axes[p][0](3))

    grads = []
    for grp in range(GROUPS):

        def backward(j, carry):
            h = grp * PER_KV + j
            gh = g[h]
            dot = jnp.sum(gh.astype(F32) * attn[h].astype(F32), axis=1, keepdims=True)
            dp = nt(gh, values_of(grp))
            dsc = (ws[h].astype(F32) * ((dp - dot) * SCALE)).astype(BF16)
            ds[j] = dsc
            dq = nn(dsc, keys_of(grp))
            cols = pl.ds(pl.multiple_of(h * HEAD, HEAD), HEAD)
            dqp[:, cols] = dq[0:PROMPT]
            dql[:, cols] = dq[PROMPT:ROWS]
            return carry

        lax.fori_loop(0, PER_KV, backward, 0)
        stack = slice(grp * PER_KV, (grp + 1) * PER_KV)
        tall = PER_KV * ROWS
        dk = tn(qs[stack].reshape(tall, HEAD), ds[...].reshape(tall, KEYS))
        dkv[grp, :, :, 0:HEAD] = dk.T.astype(BF16).reshape(PEERS, ROWS, HEAD)
        dv = tn(g[stack].reshape(tall, HEAD), ws[stack].reshape(tall, KEYS))
        dkv[grp, :, :, HEAD:256] = dv.T.astype(BF16).reshape(PEERS, ROWS, HEAD)
        if grp == 0:
            for p in (1, 2, 0):
                relay(p)
        for i, q in enumerate(peers):
            grads.append(go(dkv.at[grp, q], kin.at[grp, i], ksend.at[grp, i], krecv.at[grp, i], (leaf, q)))
    second = {}
    for p in (1, 2, 0):
        wide = PARTS[p][1]
        for i in range(4):
            direct[p, i].wait_recv()
        pad = jnp.zeros((8, wide), F32)
        for j in range(4):
            piece = slice(j * 56, (j + 1) * 56)
            full = own[p][piece] + rin[p][0, piece].astype(F32) + rin[p][1, piece].astype(F32)
            b2[p][j] = jnp.concatenate([full, pad], axis=0).astype(BF16)
        spot = spots[p][1]
        for k in (2, 1, 3):
            second[p, k] = go(b2[p].at[(spot + k) % 4], r2[p].at[k - 1], s2.at[p, k - 1], v2.at[p, k - 1], axes[p][1](k))
    third = {}
    for p in (1, 2, 0):
        for k in (1, 2, 3):
            second[p, k].wait_recv()
        full = b2[p][spots[p][1]].astype(F32)
        for k in range(3):
            full = full + r2[p][k].astype(F32)
        pad = jnp.zeros((2, PARTS[p][1]), F32)
        for j in range(4):
            piece = full[j * SHARE:(j + 1) * SHARE]
            b3[p][j] = jnp.concatenate([piece, pad], axis=0).astype(BF16)
        spot = spots[p][2]
        for k in (2, 1, 3):
            third[p, k] = go(b3[p].at[(spot + k) % 4], r3[p].at[k - 1], s3.at[p, k - 1], v3.at[p, k - 1], axes[p][2](k))
    for c in grads:
        c.wait_recv()
    for grp in range(GROUPS):
        total = dkv[grp, seq].astype(F32)
        for i in range(PEERS - 1):
            total = total + kin[grp, i].astype(F32)
        dkv_out[:, grp * HEAD:(grp + 1) * HEAD] = total[:, 0:HEAD]
        dkv_out[:, 256 + grp * HEAD:256 + (grp + 1) * HEAD] = total[:, HEAD:256]
    for p in (1, 2, 0):
        first, wide = PARTS[p]
        for k in (1, 2, 3):
            third[p, k].wait_recv()
        full = b3[p][spots[p][2]].astype(F32)
        for k in range(3):
            full = full + r3[p][k].astype(F32)
        wg[:, first:first + wide] = full[0:SHARE] * (1.0 / math.sqrt(TOKENS))
    for c in started:
        c.wait_send()


def tree_call(pq, pk, pv, lq, lk, lv, pdy, ldy, w, lengths, offsets, parents):
    any_ = pl.BlockSpec(memory_space=pl.ANY)
    vm = pl.BlockSpec(memory_space=VMEM)
    sm = pl.BlockSpec(memory_space=SMEM)
    widths = [wide for _, wide in PARTS]
    dma = pltpu.SemaphoreType.DMA
    scratch = [
        pltpu.VMEM((PEERS, ROWS, 512), BF16),
        pltpu.VMEM((ROWS, D), BF16),
        pltpu.VMEM((ROWS, D), BF16),
        pltpu.VMEM((WIDTH // 256, 256, D), BF16),
        pltpu.VMEM((HEADS, ROWS, HEAD), BF16),
        pltpu.VMEM((HEADS, ROWS, HEAD), BF16),
        pltpu.VMEM((HEADS, ROWS, HEAD), BF16),
        pltpu.VMEM((HEADS, ROWS, KEYS), BF16),
        pltpu.VMEM((PER_KV, ROWS, KEYS), BF16),
        pltpu.VMEM((WIDTH, ROWS), F32),
        pltpu.VMEM((2, 4 * CHUNK, ROWS), F32),
        pltpu.VMEM((3, 2, 4, CHUNK, ROWS), BF16),
        pltpu.VMEM((3, 4, CHUNK, ROWS), BF16),
        pltpu.VMEM((ROWS, KEYS), F32),
        pltpu.VMEM((GROUPS, PEERS, ROWS, 256), BF16),
        pltpu.VMEM((GROUPS, PEERS - 1, ROWS, 256), BF16),
    ]
    scratch += [pltpu.VMEM((CHUNK, wide), F32) for wide in widths]
    scratch += [pltpu.VMEM((2, CHUNK, wide // 2), BF16) for wide in widths]
    scratch += [pltpu.VMEM((2, CHUNK, wide), BF16) for wide in widths]
    scratch += [pltpu.VMEM((4, 64, wide), BF16) for wide in widths]
    scratch += [pltpu.VMEM((3, 64, wide), BF16) for wide in widths]
    scratch += [pltpu.VMEM((4, 16, wide), BF16) for wide in widths]
    scratch += [pltpu.VMEM((3, 16, wide), BF16) for wide in widths]
    scratch += [dma((4,)), dma((2,)), dma((WIDTH // 256,)), dma((HEADS, 2)), dma((8,)), dma((8,))]
    scratch += [dma((2,)), dma((2,)), dma((3,)), dma((3,))]
    scratch += [dma((GROUPS, PEERS - 1)), dma((GROUPS, PEERS - 1)), dma((3, 6)), dma((3, 6))]
    scratch += [dma((3, 3)), dma((3, 3)), dma((3, 3)), dma((3, 3))]
    return pl.pallas_call(
        tree_kernel,
        out_shape=(
            jax.ShapeDtypeStruct((PROMPT, WIDTH), F32),
            jax.ShapeDtypeStruct((LEAF, WIDTH), F32),
            jax.ShapeDtypeStruct((SHARE, D), F32),
            jax.ShapeDtypeStruct((ROWS, 512), F32),
        ),
        in_specs=[any_] * 9 + [sm] * 3,
        out_specs=(vm,) * 4,
        scratch_shapes=scratch,
        compiler_params=pltpu.CompilerParams(
            collective_id=0, has_side_effects=True, vmem_limit_bytes=LIMIT
        ),
        name="tree",
    )(pq, pk, pv, lq, lk, lv, pdy, ldy, w, lengths, offsets, parents)


def finish_kernel(dqp, dql, wg, dkv, pdq, pdk, pdv, ldq, ldk, ldv, out):
    pdq[...] = dqp[...]
    ldq[...] = dql[...]
    pdk[...] = dkv[0:PROMPT, 0:256]
    pdv[...] = dkv[0:PROMPT, 256:512]
    ldk[...] = dkv[PROMPT:ROWS, 0:256]
    ldv[...] = dkv[PROMPT:ROWS, 256:512]
    out[...] = wg[...]


def finish_call(dqp, dql, wg, dkv):
    vm = pl.BlockSpec(memory_space=VMEM)
    return pl.pallas_call(
        finish_kernel,
        out_shape=(
            jax.ShapeDtypeStruct((PROMPT, WIDTH), F32),
            jax.ShapeDtypeStruct((PROMPT, 256), F32),
            jax.ShapeDtypeStruct((PROMPT, 256), F32),
            jax.ShapeDtypeStruct((LEAF, WIDTH), F32),
            jax.ShapeDtypeStruct((LEAF, 256), F32),
            jax.ShapeDtypeStruct((LEAF, 256), F32),
            jax.ShapeDtypeStruct((SHARE, D), F32),
        ),
        in_specs=[vm] * 4,
        out_specs=(vm,) * 7,
        name="finish",
    )(dqp, dql, wg, dkv)


def body(pq, pk, pv, lq, lk, lv, pdy, ldy, w, lengths, offsets, parents):
    done = tree_call(
        pq[0], pk[0], pv[0], lq[0], lk[0], lv[0], pdy[0], ldy[0], w, lengths, offsets, parents
    )
    outs = finish_call(*done)
    return tuple(o[None] for o in outs[0:6]) + (outs[6],)


def solution(mesh):
    rows = P("leaf", "seq", None)
    placed = (rows,) * 8 + (P(),) + (P("leaf", None),) * 3
    return jax.shard_map(
        body,
        mesh=mesh,
        in_specs=placed,
        out_specs=(rows,) * 6 + (P(("leaf", "seq"), None),),
        check_vma=False,
    )
```

```python
import math

import jax
import jax.numpy as jnp
from jax import lax
from jax.experimental import pallas as pl
from jax.experimental.pallas import tpu as pltpu
from jax.sharding import PartitionSpec as P

MESH = pl.DeviceIdType.MESH
HEAD = 128
HEADS = 14
GROUPS = 2
PER_KV = 7
WIDTH = HEADS * HEAD
D = 3584
PROMPT = 128
LEAF = 48
ROWS = PROMPT + LEAF
PEERS = 8
KEYS = PEERS * ROWS
TOKENS = 16 * KEYS
SHARE = 14
BRANCHES = 16
CHUNK = 16 * SHARE
SCALE = 1.0 / math.sqrt(HEAD)
LOG2E = 1.0 / math.log(2.0)
NEG = -1e30
GATHERED = 2048
PARTS = ((0, 1024), (1024, 1024), (2048, 768), (2816, 768))
VMEM = pltpu.MemorySpace.VMEM
SMEM = pltpu.MemorySpace.SMEM
HALF = 256
LIMIT = 63 * 1024 * 1024
F32 = jnp.float32
BF16 = jnp.bfloat16


def nt(a, b):
    return lax.dot_general(a, b, (((1,), (1,)), ((), ())), preferred_element_type=F32)


def nn(a, b):
    return lax.dot_general(a, b, (((1,), (0,)), ((), ())), preferred_element_type=F32)


def tn(a, b):
    return lax.dot_general(a, b, (((0,), (0,)), ((), ())), preferred_element_type=F32)


def send_to(src, dst, send_sem, recv_sem, device):
    return pltpu.make_async_remote_copy(
        src_ref=src,
        dst_ref=dst,
        send_sem=send_sem,
        recv_sem=recv_sem,
        device_id=device,
        device_id_type=MESH,
    )


def flip(value, bit):
    low = (value // bit) % 2
    return value + bit - 2 * bit * low


def seq_peers(seq):
    found = []
    for d in range(1, PEERS):
        p = seq
        for bit in (1, 2, 4):
            if d & bit:
                p = flip(p, bit)
        found.append(p)
    return found


def visibility(lengths, offsets, parents, seq, bias):
    rows = lax.broadcasted_iota(jnp.int32, (ROWS, 1), 0)
    is_leaf = rows >= PROMPT
    query = jnp.where(is_leaf, seq * LEAF + rows - PROMPT, seq * PROMPT + rows)
    cols = lax.broadcasted_iota(jnp.int32, (1, KEYS), 1)
    slot = jnp.zeros((1, KEYS), jnp.int32)
    for s in range(1, PEERS):
        slot = slot + (cols >= s * ROWS).astype(jnp.int32)
    spot = cols - slot * ROWS
    key_leaf = spot >= PROMPT
    key = jnp.where(key_leaf, slot * LEAF + spot - PROMPT, slot * PROMPT + spot)
    key_branch = jnp.zeros((1, KEYS), jnp.int32)
    query_branch = jnp.zeros((ROWS, 1), jnp.int32)
    end = jnp.int32(0)
    for b in range(BRANCHES):
        end = end + lengths[0, b]
        key_branch = key_branch + (key >= end).astype(jnp.int32)
        query_branch = query_branch + (query >= end).astype(jnp.int32)
    fork = jnp.zeros((ROWS, 1), jnp.int32)
    ancestor = jnp.zeros((ROWS, 1), jnp.int32)
    for b in range(BRANCHES):
        here = query_branch == b
        fork = jnp.where(here, offsets[0, b], fork)
        ancestor = jnp.where(here, parents[0, b], ancestor)
    ancestor = jnp.where(is_leaf & (ancestor != query_branch), ancestor, -1)
    branch = jnp.where(is_leaf, query_branch, -1)
    reach = jnp.where(is_leaf, fork, query + 1)
    prompt_key = jnp.where(key_leaf, 1 << 20, key)
    key_branch = jnp.where(key_leaf, key_branch, -2)
    sees = prompt_key < reach
    sees = sees | ((key_branch == branch) & (key <= query))
    sees = sees | (key_branch == ancestor)
    bias[...] = jnp.where(sees, 0.0, NEG)


def tree_kernel(
    pq, pk, pv, lq, lk, lv, pdy, ldy, w, lengths, offsets, parents,
    dqp, dql, wg, dkv_out, *scratch
):
    (kv, yo, yt, wbuf, g, qs, attn, ws, ds, at, perm, atn, atp, ap, ag, yg, bias, dkv, kin, sa, sb) = scratch[0:21]
    own = dict(zip((2, 3), scratch[21:23]))
    rel = dict(zip((2, 3), scratch[23:25]))
    rin = dict(zip((2, 3), scratch[25:27]))
    b2 = scratch[27:31]
    r2 = scratch[31:35]
    b3 = scratch[35:39]
    r3 = scratch[39:43]
    (lsem, dsem, wsem, qsem, gsend, grecv, ysend, yrecv, psend, precv, esend, erecv, asend, arecv,
     ksend, krecv, s1, v1, s2, v2, s3, v3) = scratch[43:]
    leaf = lax.axis_index("leaf")
    seq = lax.axis_index("seq")
    core = leaf % 2
    y = leaf // 4
    plane = seq // 4
    z = ((leaf // 2) % 2) * 2 + plane
    x = seq % 4
    twin = (flip(leaf, 1), seq)
    peers = seq_peers(seq)

    def slot(q, k):
        return q * 4 + (x + k) % 4

    def on_x(k):
        return (leaf, slot(plane, k))

    def on_y(k):
        return (((y + k) % 4) * 4 + leaf % 4, seq)

    def on_z(k):
        other = (z + k) % 4
        return (y * 4 + (other // 2) * 2 + core, (other % 2) * 4 + x)

    across = (leaf, slot(1 - plane, 0))
    def on_y_core(k, c):
        return (((y + k) % 4) * 4 + ((leaf // 2) % 2) * 2 + c, seq)

    axes = ((on_y, on_z, on_x), (on_y, on_x, on_z), (on_x, on_y, on_z), (on_z, on_y, on_x))
    spots = ((y, z, x), (y, x, z), (x, y, z), (z, y, x))

    mine = [
        pltpu.make_async_copy(pk, kv.at[seq, 0:PROMPT, 0:256], lsem.at[0]),
        pltpu.make_async_copy(pv, kv.at[seq, 0:PROMPT, 256:512], lsem.at[1]),
        pltpu.make_async_copy(lk, kv.at[seq, PROMPT:ROWS, 0:256], lsem.at[2]),
        pltpu.make_async_copy(lv, kv.at[seq, PROMPT:ROWS, 256:512], lsem.at[3]),
    ]
    for c in mine:
        c.start()
    ups = [
        pltpu.make_async_copy(pdy, yo.at[0:PROMPT], dsem.at[0]),
        pltpu.make_async_copy(ldy, yo.at[PROMPT:ROWS], dsem.at[1]),
    ]
    for c in ups:
        c.start()
    tiles = WIDTH // 256
    for t in range(tiles):
        pltpu.make_async_copy(w.at[t * 256:(t + 1) * 256], wbuf.at[t], wsem.at[t]).start()
    queries = []
    for h in range(HEADS):
        cols = slice(h * HEAD, (h + 1) * HEAD)
        queries.append(pltpu.make_async_copy(pq.at[:, cols], qs.at[h, 0:PROMPT], qsem.at[h, 0]))
        queries.append(pltpu.make_async_copy(lq.at[:, cols], qs.at[h, PROMPT:ROWS], qsem.at[h, 1]))
    for c in queries:
        c.start()
    barrier = pltpu.get_barrier_semaphore()
    greet = [(leaf, p) for p in peers] + [twin]
    greet += [on_y(k) for k in (1, 2, 3)] + [on_z(k) for k in (1, 2, 3)]
    greet += [on_y_core(k, 1 - core) for k in (1, 2, 3)]
    for d in greet:
        pl.semaphore_signal(barrier, inc=1, device_id=d, device_id_type=MESH)
    pl.semaphore_wait(barrier, len(greet))
    started = []

    def go(src, dst, send_sem, recv_sem, device):
        c = send_to(src, dst, send_sem, recv_sem, device)
        c.start()
        started.append(c)
        return c

    def pass_on(ref, i, device):
        return go(ref, ref, gsend.at[i], grecv.at[i], device)

    def arrived(ref, i):
        send_to(ref, ref, gsend.at[i], grecv.at[i], across).wait_recv()

    for c in mine:
        c.wait()
    block = kv.at[seq]
    pass_on(block, 0, across)
    pass_on(block, 1, on_x(1))
    pass_on(block, 2, on_x(3))
    swaps = [
        go(pdy, yt.at[0:PROMPT], ysend.at[0], yrecv.at[0], twin),
        go(ldy, yt.at[PROMPT:ROWS], ysend.at[1], yrecv.at[1], twin),
    ]
    for c in ups:
        c.wait()

    def strip(src, dst, i, device):
        return go(src, dst, psend.at[i], precv.at[i], device)

    def came(dst, i):
        send_to(dst, dst, psend.at[i], precv.at[i], twin).wait_recv()

    quarter = GATHERED // 2
    strip(yo.at[:, 0:GATHERED], yg.at[2, core], 0, on_y(1))
    strip(yo.at[:, 0:GATHERED], yg.at[0, core], 1, on_y(3))

    def tile(t, carry):
        pltpu.make_async_copy(w.at[0:256], wbuf.at[t], wsem.at[t]).wait()
        acc = nt(yo[...], wbuf[t]).astype(BF16)
        g[2 * t] = acc[:, 0:HEAD]
        g[2 * t + 1] = acc[:, HEAD:256]
        return carry

    lax.fori_loop(0, tiles, tile, 0)
    arrived(kv.at[slot(plane, 3)], 1)
    pass_on(kv.at[slot(plane, 3), :, 0:HALF], 3, on_x(1))
    arrived(kv.at[slot(plane, 1)], 2)
    pass_on(kv.at[slot(plane, 1), :, HALF:512], 4, on_x(3))
    arrived(kv.at[slot(1 - plane, 0)], 0)
    pass_on(kv.at[slot(1 - plane, 0)], 5, on_x(1))
    pass_on(kv.at[slot(1 - plane, 0)], 6, on_x(3))
    visibility(lengths, offsets, parents, seq, bias)
    arrived(kv.at[slot(plane, 2), :, 0:HALF], 3)
    arrived(kv.at[slot(plane, 2), :, HALF:512], 4)
    pass_on(kv.at[slot(plane, 2)], 7, across)
    for c in queries:
        c.wait()
    arrived(kv.at[slot(1 - plane, 3)], 5)
    arrived(kv.at[slot(1 - plane, 1)], 6)
    arrived(kv.at[slot(1 - plane, 2)], 7)

    def keys_of(grp):
        cols = pl.ds(pl.multiple_of(grp * HEAD, HEAD), HEAD)
        return kv[:, :, cols].reshape(KEYS, HEAD)

    def values_of(grp):
        cols = pl.ds(pl.multiple_of(256 + grp * HEAD, HEAD), HEAD)
        return kv[:, :, cols].reshape(KEYS, HEAD)

    def score(h, out):
        out[...] = nt(qs[h], keys_of(h // PER_KV))

    def soften(h, src):
        for r in range(0, ROWS, 16):
            here = slice(r, r + 16)
            t = src[here] * (SCALE * LOG2E) + bias[here]
            e = jnp.exp2(t - jnp.max(t, axis=1, keepdims=True))
            share = 1.0 / jnp.sum(e, axis=1, keepdims=True)
            ws[h, here] = (e * share).astype(BF16)

    def attend(h):
        a = nn(ws[h], values_of(h // PER_KV)).astype(BF16)
        attn[h] = a
        at[pl.ds(pl.multiple_of(h * HEAD, HEAD), HEAD), :] = a.astype(F32).T

    def forward(i, carry):
        score(2 * i + 1, sb)
        soften(2 * i, sa)
        score(jnp.minimum(2 * i + 2, HEADS - 1), sa)
        attend(2 * i)
        soften(2 * i + 1, sb)
        attend(2 * i + 1)
        return carry

    score(0, sa)
    lax.fori_loop(0, 4, forward, 0)
    came(yg.at[2, core], 0)
    strip(yg.at[2, core, :, 0:quarter], yg.at[1, core, :, 0:quarter], 2, on_y(1))
    came(yg.at[0, core], 1)
    strip(yg.at[0, core, :, quarter:GATHERED], yg.at[1, core, :, quarter:GATHERED], 3, on_y(3))
    strip(yg.at[2, core], yg.at[2, core], 4, twin)
    strip(yg.at[0, core], yg.at[0, core], 5, twin)
    lax.fori_loop(4, HEADS // 2, forward, 0)
    for c in range(2):
        for yy in range(4):
            for zh in range(2):
                n = yy * 448 + zh * 224 + c * 112
                atn[c, yy, zh * 112:(zh + 1) * 112, :] = at[n:n + 112, :].astype(BF16)
    for k in (2, 1, 3):
        for c in range(2):
            go(atn.at[c, (y + k) % 4], ag.at[4 - k, core], esend.at[k, c], erecv.at[4 - k, core], on_y_core(k, c))
    go(atn.at[1 - core, y], ag.at[0, core], esend.at[0, 0], erecv.at[0, core], twin)
    for c in range(2):
        for yy in range(4):
            for zz in range(4):
                n = yy * 448 + (zz // 2) * 224 + c * 112 + (zz % 2) * 56
                r = zz * CHUNK + yy * 56
                perm[1, r:r + 56, :] = at[n:n + 56, :]
                for xx in range(4):
                    r = xx * CHUNK + yy * 56 + zz * SHARE
                    perm[0, r:r + SHARE, :] = at[n + xx * SHARE:n + (xx + 1) * SHARE, :]
        for k in range(4):
            atp[0, c, k] = perm[0, k * CHUNK:(k + 1) * CHUNK, :].astype(BF16)
            atp[1, c, k] = perm[1, k * CHUNK:(k + 1) * CHUNK, :].astype(BF16)
    rows = []
    for p in range(2):
        rows.append(go(atp.at[p, 1 - core], ap.at[p], asend.at[p], arecv.at[p], twin))
    came(yg.at[1, core, :, 0:quarter], 2)
    came(yg.at[1, core, :, quarter:GATHERED], 3)
    strip(yg.at[1, core], yg.at[1, core], 6, twin)
    for c in swaps:
        c.wait_recv()
    for c in rows:
        c.wait_recv()

    def part(p, k, lo, hi):
        first = PARTS[p][0]
        return wbuf.at[k, 0:CHUNK, first + lo:first + hi]

    def product(p, k):
        first, wide = PARTS[p]
        dest = (spots[p][0] + k) % 4
        cols = slice(first, first + wide)
        return nn(atp[p - 2, core, dest], yo[:, cols]) + nn(ap[p - 2, dest], yt[:, cols])

    relays = {}
    direct = {}
    for p in (2, 3):
        wide = PARTS[p][1]
        h = wide // 2
        part(p, 2, 0, wide)[...] = product(p, 2).astype(BF16)
        relays[p, 0] = go(part(p, 2, 0, h), rel[p].at[0], s1.at[p - 2, 0], v1.at[p - 2, 0], axes[p][0](1))
        relays[p, 1] = go(part(p, 2, h, wide), rel[p].at[1], s1.at[p - 2, 1], v1.at[p - 2, 1], axes[p][0](3))
    for p in (2, 3):
        wide = PARTS[p][1]
        h = wide // 2
        part(p, 1, 0, wide)[...] = product(p, 1).astype(BF16)
        direct[p, 0] = go(part(p, 1, h, wide), rin[p].at[0, :, h:wide], s1.at[p - 2, 2], v1.at[p - 2, 2], axes[p][0](1))
        part(p, 3, 0, wide)[...] = product(p, 3).astype(BF16)
        direct[p, 1] = go(part(p, 3, 0, h), rin[p].at[1, :, 0:h], s1.at[p - 2, 3], v1.at[p - 2, 3], axes[p][0](3))
    for p in (2, 3):
        own[p][...] = product(p, 0)

    def relay(p):
        wide = PARTS[p][1]
        h = wide // 2
        relays[p, 0].wait_recv()
        here = part(p, 1, 0, h)
        here[...] = (here[...].astype(F32) + rel[p][0].astype(F32)).astype(BF16)
        direct[p, 2] = go(here, rin[p].at[0, :, 0:h], s1.at[p - 2, 4], v1.at[p - 2, 4], axes[p][0](1))
        relays[p, 1].wait_recv()
        here = part(p, 3, h, wide)
        here[...] = (here[...].astype(F32) + rel[p][1].astype(F32)).astype(BF16)
        direct[p, 3] = go(here, rin[p].at[1, :, h:wide], s1.at[p - 2, 5], v1.at[p - 2, 5], axes[p][0](3))

    def heads_back(grp):
        def backward(j, carry):
            h = grp * PER_KV + j
            gh = g[h]
            dot = jnp.sum(gh.astype(F32) * attn[h].astype(F32), axis=1, keepdims=True)
            dp = nt(gh, values_of(grp))
            dsc = (ws[h].astype(F32) * (dp - dot)).astype(BF16)
            ds[j] = dsc
            dq = nn(dsc, keys_of(grp)) * SCALE
            cols = pl.ds(pl.multiple_of(h * HEAD, HEAD), HEAD)
            dqp[:, cols] = dq[0:PROMPT]
            dql[:, cols] = dq[PROMPT:ROWS]
            return carry

        lax.fori_loop(0, PER_KV, backward, 0)

    def keys_back(grp):
        stack = slice(grp * PER_KV, (grp + 1) * PER_KV)
        tall = PER_KV * ROWS
        dk = tn(qs[stack].reshape(tall, HEAD), ds[...].reshape(tall, KEYS)) * SCALE
        dkv[grp, :, :, 0:HEAD] = dk.T.astype(BF16).reshape(PEERS, ROWS, HEAD)
        dv = tn(g[stack].reshape(tall, HEAD), ws[stack].reshape(tall, KEYS))
        dkv[grp, :, :, HEAD:256] = dv.T.astype(BF16).reshape(PEERS, ROWS, HEAD)

    def hop(grp, i, src, dst, device):
        return go(src, dst, ksend.at[grp, i], krecv.at[grp, i], device)

    hops = {}

    def add_in(grp, q, cols, i):
        here = dkv.at[grp, q, :, cols]
        here[...] = (here[...].astype(F32) + kin[grp, i, :, cols].astype(F32)).astype(BF16)

    left, right, whole = slice(0, HEAD), slice(HEAD, 256), slice(0, 256)

    def grads_one(grp):
        hops[grp, 0] = hop(grp, 0, dkv.at[grp, slot(1 - plane, 2)], kin.at[grp, 0], across)
        hops[grp, 1] = hop(grp, 1, dkv.at[grp, slot(1 - plane, 1)], kin.at[grp, 1], on_x(1))
        hops[grp, 2] = hop(grp, 2, dkv.at[grp, slot(1 - plane, 3)], kin.at[grp, 2], on_x(3))

    def grads_two(grp):
        hops[grp, 0].wait_recv()
        far = slot(plane, 2)
        add_in(grp, far, whole, 0)
        hops[grp, 3] = hop(grp, 3, dkv.at[grp, far, :, left], kin.at[grp, 3, :, left], on_x(1))
        hops[grp, 4] = hop(grp, 4, dkv.at[grp, far, :, right], kin.at[grp, 3, :, right], on_x(3))
        hops[grp, 1].wait_recv()
        hops[grp, 2].wait_recv()
        near = slot(1 - plane, 0)
        total = dkv[grp, near].astype(F32) + kin[grp, 1].astype(F32) + kin[grp, 2].astype(F32)
        dkv[grp, near] = total.astype(BF16)
        hops[grp, 7] = hop(grp, 7, dkv.at[grp, near], kin.at[grp, 4], across)

    def grads_three(grp):
        hops[grp, 3].wait_recv()
        add_in(grp, slot(plane, 1), left, 3)
        hops[grp, 5] = hop(grp, 5, dkv.at[grp, slot(plane, 1)], kin.at[grp, 5], on_x(1))
        hops[grp, 4].wait_recv()
        add_in(grp, slot(plane, 3), right, 3)
        hops[grp, 6] = hop(grp, 6, dkv.at[grp, slot(plane, 3)], kin.at[grp, 6], on_x(3))

    def grads_last(grp):
        total = dkv[grp, seq].astype(F32)
        for i in (7, 5, 6):
            hops[grp, i].wait_recv()
        for i in (4, 5, 6):
            total = total + kin[grp, i].astype(F32)
        dkv_out[:, grp * HEAD:(grp + 1) * HEAD] = total[:, 0:HEAD]
        dkv_out[:, 256 + grp * HEAD:256 + (grp + 1) * HEAD] = total[:, HEAD:256]

    second = {}
    third = {}

    def send_second(p, pieces):
        pad = jnp.zeros((8, PARTS[p][1]), F32)
        for j in range(4):
            b2[p][j] = jnp.concatenate([pieces[j], pad], axis=0).astype(BF16)
        spot = spots[p][1]
        for k in (2, 1, 3):
            second[p, k] = go(b2[p].at[(spot + k) % 4], r2[p].at[k - 1], s2.at[p, k - 1], v2.at[p, k - 1], axes[p][1](k))

    def gathered(p):
        first, wide = PARTS[p]
        cols = slice(first, first + wide)
        full = nn(atn[core, y], yo[:, cols]) + nn(ag[0, 1 - core], yt[:, cols])
        for k in (1, 3, 2):
            for c in range(2):
                full = full + nn(ag[k, c], yg[k - 1, c, :, cols])
        if p == 0:
            send_second(p, [full[j * 56:(j + 1) * 56] for j in range(4)])
        else:
            strips = []
            for j in range(4):
                rows_of = [full[zz * 56 + j * SHARE:zz * 56 + (j + 1) * SHARE] for zz in range(4)]
                strips.append(jnp.concatenate(rows_of, axis=0))
            send_second(p, strips)

    def scattered(p):
        for i in range(4):
            direct[p, i].wait_recv()
        pieces = []
        for j in range(4):
            piece = slice(j * 56, (j + 1) * 56)
            pieces.append(own[p][piece] + rin[p][0, piece].astype(F32) + rin[p][1, piece].astype(F32))
        send_second(p, pieces)

    def send_third(p):
        for k in (1, 2, 3):
            second[p, k].wait_recv()
        full = b2[p][spots[p][1]].astype(F32)
        for k in range(3):
            full = full + r2[p][k].astype(F32)
        pad = jnp.zeros((2, PARTS[p][1]), F32)
        for j in range(4):
            piece = full[j * SHARE:(j + 1) * SHARE]
            b3[p][j] = jnp.concatenate([piece, pad], axis=0).astype(BF16)
        spot = spots[p][2]
        for k in (2, 1, 3):
            third[p, k] = go(b3[p].at[(spot + k) % 4], r3[p].at[k - 1], s3.at[p, k - 1], v3.at[p, k - 1], axes[p][2](k))

    heads_back(0)
    relay(2)
    relay(3)
    keys_back(0)
    grads_one(0)
    send_to(ag.at[0, 1 - core], ag.at[0, 1 - core], esend.at[0, 0], erecv.at[0, 1 - core], twin).wait_recv()
    for k in (1, 2, 3):
        for c in range(2):
            send_to(ag.at[k, c], ag.at[k, c], esend.at[k, c], erecv.at[k, c], twin).wait_recv()
    came(yg.at[2, 1 - core], 4)
    came(yg.at[0, 1 - core], 5)
    came(yg.at[1, 1 - core], 6)
    gathered(0)
    gathered(1)
    heads_back(1)
    scattered(2)
    scattered(3)
    keys_back(1)
    grads_one(1)
    grads_two(0)
    send_third(0)
    send_third(1)
    grads_two(1)
    grads_three(0)
    send_third(2)
    send_third(3)
    grads_three(1)
    grads_last(0)
    for p in range(4):
        first, wide = PARTS[p]
        for k in (1, 2, 3):
            third[p, k].wait_recv()
        full = b3[p][spots[p][2]].astype(F32)
        for k in range(3):
            full = full + r3[p][k].astype(F32)
        wg[:, first:first + wide] = full[0:SHARE] * (1.0 / math.sqrt(TOKENS))
    grads_last(1)
    for c in started:
        c.wait_send()


def tree_call(pq, pk, pv, lq, lk, lv, pdy, ldy, w, lengths, offsets, parents):
    any_ = pl.BlockSpec(memory_space=pl.ANY)
    vm = pl.BlockSpec(memory_space=VMEM)
    sm = pl.BlockSpec(memory_space=SMEM)
    widths = [wide for _, wide in PARTS]
    dma = pltpu.SemaphoreType.DMA
    scratch = [
        pltpu.VMEM((PEERS, ROWS, 512), BF16),
        pltpu.VMEM((ROWS, D), BF16),
        pltpu.VMEM((ROWS, D), BF16),
        pltpu.VMEM((WIDTH // 256, 256, D), BF16),
        pltpu.VMEM((HEADS, ROWS, HEAD), BF16),
        pltpu.VMEM((HEADS, ROWS, HEAD), BF16),
        pltpu.VMEM((HEADS, ROWS, HEAD), BF16),
        pltpu.VMEM((HEADS, ROWS, KEYS), BF16),
        pltpu.VMEM((PER_KV, ROWS, KEYS), BF16),
        pltpu.VMEM((WIDTH, ROWS), F32),
        pltpu.VMEM((2, 4 * CHUNK, ROWS), F32),
        pltpu.VMEM((2, 4, CHUNK, ROWS), BF16),
        pltpu.VMEM((2, 2, 4, CHUNK, ROWS), BF16),
        pltpu.VMEM((2, 4, CHUNK, ROWS), BF16),
        pltpu.VMEM((4, 2, CHUNK, ROWS), BF16),
        pltpu.VMEM((3, 2, ROWS, GATHERED), BF16),
        pltpu.VMEM((ROWS, KEYS), F32),
        pltpu.VMEM((GROUPS, PEERS, ROWS, 256), BF16),
        pltpu.VMEM((GROUPS, 7, ROWS, 256), BF16),
        pltpu.VMEM((ROWS, KEYS), F32),
        pltpu.VMEM((ROWS, KEYS), F32),
    ]
    late = widths[2:]
    scratch += [pltpu.VMEM((CHUNK, wide), F32) for wide in late]
    scratch += [pltpu.VMEM((2, CHUNK, wide // 2), BF16) for wide in late]
    scratch += [pltpu.VMEM((2, CHUNK, wide), BF16) for wide in late]
    scratch += [pltpu.VMEM((4, 64, wide), BF16) for wide in widths]
    scratch += [pltpu.VMEM((3, 64, wide), BF16) for wide in widths]
    scratch += [pltpu.VMEM((4, 16, wide), BF16) for wide in widths]
    scratch += [pltpu.VMEM((3, 16, wide), BF16) for wide in widths]
    scratch += [dma((4,)), dma((2,)), dma((WIDTH // 256,)), dma((HEADS, 2)), dma((8,)), dma((8,))]
    scratch += [dma((2,)), dma((2,)), dma((7,)), dma((7,)), dma((4, 2)), dma((4, 2)), dma((2,)), dma((2,))]
    scratch += [dma((GROUPS, 8)), dma((GROUPS, 8)), dma((2, 6)), dma((2, 6))]
    scratch += [dma((4, 3)), dma((4, 3)), dma((4, 3)), dma((4, 3))]
    return pl.pallas_call(
        tree_kernel,
        out_shape=(
            jax.ShapeDtypeStruct((PROMPT, WIDTH), F32),
            jax.ShapeDtypeStruct((LEAF, WIDTH), F32),
            jax.ShapeDtypeStruct((SHARE, D), F32),
            jax.ShapeDtypeStruct((ROWS, 512), F32),
        ),
        in_specs=[any_] * 9 + [sm] * 3,
        out_specs=(vm,) * 4,
        scratch_shapes=scratch,
        compiler_params=pltpu.CompilerParams(
            collective_id=0, has_side_effects=True, vmem_limit_bytes=LIMIT
        ),
        name="tree",
    )(pq, pk, pv, lq, lk, lv, pdy, ldy, w, lengths, offsets, parents)


def finish_kernel(dqp, dql, wg, dkv, pdq, pdk, pdv, ldq, ldk, ldv, out):
    pdq[...] = dqp[...]
    ldq[...] = dql[...]
    pdk[...] = dkv[0:PROMPT, 0:256]
    pdv[...] = dkv[0:PROMPT, 256:512]
    ldk[...] = dkv[PROMPT:ROWS, 0:256]
    ldv[...] = dkv[PROMPT:ROWS, 256:512]
    out[...] = wg[...]


def finish_call(dqp, dql, wg, dkv):
    vm = pl.BlockSpec(memory_space=VMEM)
    return pl.pallas_call(
        finish_kernel,
        out_shape=(
            jax.ShapeDtypeStruct((PROMPT, WIDTH), F32),
            jax.ShapeDtypeStruct((PROMPT, 256), F32),
            jax.ShapeDtypeStruct((PROMPT, 256), F32),
            jax.ShapeDtypeStruct((LEAF, WIDTH), F32),
            jax.ShapeDtypeStruct((LEAF, 256), F32),
            jax.ShapeDtypeStruct((LEAF, 256), F32),
            jax.ShapeDtypeStruct((SHARE, D), F32),
        ),
        in_specs=[vm] * 4,
        out_specs=(vm,) * 7,
        name="finish",
    )(dqp, dql, wg, dkv)


def body(pq, pk, pv, lq, lk, lv, pdy, ldy, w, lengths, offsets, parents):
    done = tree_call(
        pq[0], pk[0], pv[0], lq[0], lk[0], lv[0], pdy[0], ldy[0], w, lengths, offsets, parents
    )
    outs = finish_call(*done)
    return tuple(o[None] for o in outs[0:6]) + (outs[6],)


def solution(mesh):
    rows = P("leaf", "seq", None)
    placed = (rows,) * 8 + (P(),) + (P("leaf", None),) * 3
    return jax.shard_map(
        body,
        mesh=mesh,
        in_specs=placed,
        out_specs=(rows,) * 6 + (P(("leaf", "seq"), None),),
        check_vma=False,
    )
```

```python
import math

import jax
import jax.numpy as jnp
from jax import lax
from jax.experimental import pallas as pl
from jax.experimental.pallas import tpu as pltpu
from jax.sharding import PartitionSpec as P

MESH = pl.DeviceIdType.MESH
HEAD = 128
HEADS = 14
GROUPS = 2
PER_KV = 7
WIDTH = HEADS * HEAD
D = 3584
PROMPT = 128
LEAF = 48
ROWS = PROMPT + LEAF
PEERS = 8
KEYS = PEERS * ROWS
TOKENS = 16 * KEYS
SHARE = 14
BRANCHES = 16
CHUNK = 16 * SHARE
SCALE = 1.0 / math.sqrt(HEAD)
LOG2E = 1.0 / math.log(2.0)
NEG = -1e30
GATHERED = 2048
PARTS = ((0, 1024), (1024, 1024), (2048, 768), (2816, 768))
VMEM = pltpu.MemorySpace.VMEM
SMEM = pltpu.MemorySpace.SMEM
HALF = 256
LIMIT = 63 * 1024 * 1024
F32 = jnp.float32
BF16 = jnp.bfloat16


def nt(a, b):
    return lax.dot_general(a, b, (((1,), (1,)), ((), ())), preferred_element_type=F32)


def nn(a, b):
    return lax.dot_general(a, b, (((1,), (0,)), ((), ())), preferred_element_type=F32)


def tn(a, b):
    return lax.dot_general(a, b, (((0,), (0,)), ((), ())), preferred_element_type=F32)


def send_to(src, dst, send_sem, recv_sem, device):
    return pltpu.make_async_remote_copy(
        src_ref=src,
        dst_ref=dst,
        send_sem=send_sem,
        recv_sem=recv_sem,
        device_id=device,
        device_id_type=MESH,
    )


def flip(value, bit):
    low = (value // bit) % 2
    return value + bit - 2 * bit * low


def seq_peers(seq):
    found = []
    for d in range(1, PEERS):
        p = seq
        for bit in (1, 2, 4):
            if d & bit:
                p = flip(p, bit)
        found.append(p)
    return found


def visibility(lengths, offsets, parents, seq, bias):
    rows = lax.broadcasted_iota(jnp.int32, (ROWS, 1), 0)
    is_leaf = rows >= PROMPT
    query = jnp.where(is_leaf, seq * LEAF + rows - PROMPT, seq * PROMPT + rows)
    cols = lax.broadcasted_iota(jnp.int32, (1, KEYS), 1)
    slot = jnp.zeros((1, KEYS), jnp.int32)
    for s in range(1, PEERS):
        slot = slot + (cols >= s * ROWS).astype(jnp.int32)
    spot = cols - slot * ROWS
    key_leaf = spot >= PROMPT
    key = jnp.where(key_leaf, slot * LEAF + spot - PROMPT, slot * PROMPT + spot)
    key_branch = jnp.zeros((1, KEYS), jnp.int32)
    query_branch = jnp.zeros((ROWS, 1), jnp.int32)
    end = jnp.int32(0)
    for b in range(BRANCHES):
        end = end + lengths[0, b]
        key_branch = key_branch + (key >= end).astype(jnp.int32)
        query_branch = query_branch + (query >= end).astype(jnp.int32)
    fork = jnp.zeros((ROWS, 1), jnp.int32)
    ancestor = jnp.zeros((ROWS, 1), jnp.int32)
    for b in range(BRANCHES):
        here = query_branch == b
        fork = jnp.where(here, offsets[0, b], fork)
        ancestor = jnp.where(here, parents[0, b], ancestor)
    ancestor = jnp.where(is_leaf & (ancestor != query_branch), ancestor, -1)
    branch = jnp.where(is_leaf, query_branch, -1)
    reach = jnp.where(is_leaf, fork, query + 1)
    prompt_key = jnp.where(key_leaf, 1 << 20, key)
    key_branch = jnp.where(key_leaf, key_branch, -2)
    sees = prompt_key < reach
    sees = sees | ((key_branch == branch) & (key <= query))
    sees = sees | (key_branch == ancestor)
    bias[...] = jnp.where(sees, 0.0, NEG)


def tree_kernel(
    pq, pk, pv, lq, lk, lv, pdy, ldy, w, lengths, offsets, parents,
    dqp, dql, wg, dkv_out, *scratch
):
    (kv, yo, yt, wbuf, g, qs, attn, ws, ds, at, perm, atn, atp, ap, ag, yg, bias, dkv, kin, sa, sb) = scratch[0:21]
    own = dict(zip((2, 3), scratch[21:23]))
    rel = dict(zip((2, 3), scratch[23:25]))
    rin = dict(zip((2, 3), scratch[25:27]))
    b2 = scratch[27:31]
    r2 = scratch[31:35]
    b3 = scratch[35:39]
    r3 = scratch[39:43]
    (lsem, dsem, wsem, qsem, gsend, grecv, ysend, yrecv, psend, precv, esend, erecv, asend, arecv,
     ksend, krecv, s1, v1, s2, v2, s3, v3) = scratch[43:]
    leaf = lax.axis_index("leaf")
    seq = lax.axis_index("seq")
    core = leaf % 2
    y = leaf // 4
    plane = seq // 4
    z = ((leaf // 2) % 2) * 2 + plane
    x = seq % 4
    twin = (flip(leaf, 1), seq)
    peers = seq_peers(seq)

    def slot(q, k):
        return q * 4 + (x + k) % 4

    def on_x(k):
        return (leaf, slot(plane, k))

    def on_y(k):
        return (((y + k) % 4) * 4 + leaf % 4, seq)

    def on_z(k):
        other = (z + k) % 4
        return (y * 4 + (other // 2) * 2 + core, (other % 2) * 4 + x)

    across = (leaf, slot(1 - plane, 0))
    def on_y_core(k, c):
        return (((y + k) % 4) * 4 + ((leaf // 2) % 2) * 2 + c, seq)

    axes = ((on_y, on_z, on_x), (on_y, on_x, on_z), (on_x, on_y, on_z), (on_z, on_y, on_x))
    spots = ((y, z, x), (y, x, z), (x, y, z), (z, y, x))

    mine = [
        pltpu.make_async_copy(pk, kv.at[seq, 0:PROMPT, 0:256], lsem.at[0]),
        pltpu.make_async_copy(pv, kv.at[seq, 0:PROMPT, 256:512], lsem.at[1]),
        pltpu.make_async_copy(lk, kv.at[seq, PROMPT:ROWS, 0:256], lsem.at[2]),
        pltpu.make_async_copy(lv, kv.at[seq, PROMPT:ROWS, 256:512], lsem.at[3]),
    ]
    for c in mine:
        c.start()
    ups = [
        pltpu.make_async_copy(pdy, yo.at[0:PROMPT], dsem.at[0]),
        pltpu.make_async_copy(ldy, yo.at[PROMPT:ROWS], dsem.at[1]),
    ]
    for c in ups:
        c.start()
    tiles = WIDTH // 256
    for t in range(tiles):
        pltpu.make_async_copy(w.at[t * 256:(t + 1) * 256], wbuf.at[t], wsem.at[t]).start()
    queries = []
    for h in range(HEADS):
        cols = slice(h * HEAD, (h + 1) * HEAD)
        queries.append(pltpu.make_async_copy(pq.at[:, cols], qs.at[h, 0:PROMPT], qsem.at[h, 0]))
        queries.append(pltpu.make_async_copy(lq.at[:, cols], qs.at[h, PROMPT:ROWS], qsem.at[h, 1]))
    for c in queries:
        c.start()
    barrier = pltpu.get_barrier_semaphore()
    greet = [(leaf, p) for p in peers] + [twin]
    greet += [on_y(k) for k in (1, 2, 3)] + [on_z(k) for k in (1, 2, 3)]
    greet += [on_y_core(k, 1 - core) for k in (1, 2, 3)]
    for d in greet:
        pl.semaphore_signal(barrier, inc=1, device_id=d, device_id_type=MESH)
    pl.semaphore_wait(barrier, len(greet))
    started = []

    def go(src, dst, send_sem, recv_sem, device):
        c = send_to(src, dst, send_sem, recv_sem, device)
        c.start()
        started.append(c)
        return c

    def pass_on(ref, i, device):
        return go(ref, ref, gsend.at[i], grecv.at[i], device)

    def arrived(ref, i):
        send_to(ref, ref, gsend.at[i], grecv.at[i], across).wait_recv()

    for c in mine:
        c.wait()
    block = kv.at[seq]
    pass_on(block, 0, across)
    pass_on(kv.at[seq, :, 0:HALF], 1, on_x(1))
    pass_on(kv.at[seq, :, HALF:512], 2, on_x(3))
    pass_on(kv.at[seq, :, HALF:512], 8, on_x(1))
    pass_on(kv.at[seq, :, 0:HALF], 9, on_x(3))
    swaps = [
        go(pdy, yt.at[0:PROMPT], ysend.at[0], yrecv.at[0], twin),
        go(ldy, yt.at[PROMPT:ROWS], ysend.at[1], yrecv.at[1], twin),
    ]
    for c in ups:
        c.wait()

    def strip(src, dst, i, device):
        return go(src, dst, psend.at[i], precv.at[i], device)

    def came(dst, i):
        send_to(dst, dst, psend.at[i], precv.at[i], twin).wait_recv()

    quarter = GATHERED // 2
    lower, upper = slice(0, quarter), slice(quarter, GATHERED)
    strip(yo.at[:, lower], yg.at[2, core, :, lower], 0, on_y(1))
    strip(yo.at[:, upper], yg.at[0, core, :, upper], 1, on_y(3))
    strip(yo.at[:, upper], yg.at[2, core, :, upper], 2, on_y(1))
    strip(yo.at[:, lower], yg.at[0, core, :, lower], 3, on_y(3))

    def tile(t, carry):
        pltpu.make_async_copy(w.at[0:256], wbuf.at[t], wsem.at[t]).wait()
        acc = nt(yo[...], wbuf[t]).astype(BF16)
        g[2 * t] = acc[:, 0:HEAD]
        g[2 * t + 1] = acc[:, HEAD:256]
        return carry

    lax.fori_loop(0, tiles, tile, 0)
    arrived(kv.at[slot(plane, 3), :, 0:HALF], 1)
    pass_on(kv.at[slot(plane, 3), :, 0:HALF], 3, on_x(1))
    arrived(kv.at[slot(plane, 1), :, HALF:512], 2)
    pass_on(kv.at[slot(plane, 1), :, HALF:512], 4, on_x(3))
    arrived(kv.at[slot(1 - plane, 0)], 0)
    pass_on(kv.at[slot(1 - plane, 0)], 5, on_x(1))
    pass_on(kv.at[slot(1 - plane, 0)], 6, on_x(3))
    visibility(lengths, offsets, parents, seq, bias)
    arrived(kv.at[slot(plane, 2), :, 0:HALF], 3)
    arrived(kv.at[slot(plane, 2), :, HALF:512], 4)
    pass_on(kv.at[slot(plane, 2)], 7, across)
    for c in queries:
        c.wait()
    came(yg.at[2, core, :, lower], 0)
    strip(yg.at[2, core, :, lower], yg.at[1, core, :, lower], 4, on_y(1))
    came(yg.at[0, core, :, upper], 1)
    strip(yg.at[0, core, :, upper], yg.at[1, core, :, upper], 5, on_y(3))
    arrived(kv.at[slot(plane, 3), :, HALF:512], 8)
    arrived(kv.at[slot(plane, 1), :, 0:HALF], 9)
    arrived(kv.at[slot(1 - plane, 3)], 5)
    arrived(kv.at[slot(1 - plane, 1)], 6)
    arrived(kv.at[slot(1 - plane, 2)], 7)

    def keys_of(grp):
        cols = pl.ds(pl.multiple_of(grp * HEAD, HEAD), HEAD)
        return kv[:, :, cols].reshape(KEYS, HEAD)

    def values_of(grp):
        cols = pl.ds(pl.multiple_of(256 + grp * HEAD, HEAD), HEAD)
        return kv[:, :, cols].reshape(KEYS, HEAD)

    def score(h, out):
        out[...] = nt(qs[h], keys_of(h // PER_KV))

    def soften(h, src):
        for r in range(0, ROWS, 16):
            here = slice(r, r + 16)
            t = src[here] * (SCALE * LOG2E) + bias[here]
            e = jnp.exp2(t - jnp.max(t, axis=1, keepdims=True))
            share = 1.0 / jnp.sum(e, axis=1, keepdims=True)
            ws[h, here] = (e * share).astype(BF16)

    def attend(h):
        a = nn(ws[h], values_of(h // PER_KV)).astype(BF16)
        attn[h] = a
        at[pl.ds(pl.multiple_of(h * HEAD, HEAD), HEAD), :] = a.astype(F32).T

    def forward(i, carry):
        score(2 * i + 1, sb)
        soften(2 * i, sa)
        score(jnp.minimum(2 * i + 2, HEADS - 1), sa)
        attend(2 * i)
        soften(2 * i + 1, sb)
        attend(2 * i + 1)
        return carry

    score(0, sa)
    lax.fori_loop(0, 4, forward, 0)
    came(yg.at[2, core, :, upper], 2)
    strip(yg.at[2, core], yg.at[2, core], 6, twin)
    came(yg.at[0, core, :, lower], 3)
    strip(yg.at[0, core], yg.at[0, core], 7, twin)
    lax.fori_loop(4, HEADS // 2, forward, 0)
    for c in range(2):
        for yy in range(4):
            for zh in range(2):
                n = yy * 448 + zh * 224 + c * 112
                atn[c, yy, zh * 112:(zh + 1) * 112, :] = at[n:n + 112, :].astype(BF16)
    for k in (2, 1, 3):
        for c in range(2):
            go(atn.at[c, (y + k) % 4], ag.at[4 - k, core], esend.at[k, c], erecv.at[4 - k, core], on_y_core(k, c))
    go(atn.at[1 - core, y], ag.at[0, core], esend.at[0, 0], erecv.at[0, core], twin)
    for c in range(2):
        for yy in range(4):
            for zz in range(4):
                n = yy * 448 + (zz // 2) * 224 + c * 112 + (zz % 2) * 56
                r = zz * CHUNK + yy * 56
                perm[1, r:r + 56, :] = at[n:n + 56, :]
                for xx in range(4):
                    r = xx * CHUNK + yy * 56 + zz * SHARE
                    perm[0, r:r + SHARE, :] = at[n + xx * SHARE:n + (xx + 1) * SHARE, :]
        for k in range(4):
            atp[0, c, k] = perm[0, k * CHUNK:(k + 1) * CHUNK, :].astype(BF16)
            atp[1, c, k] = perm[1, k * CHUNK:(k + 1) * CHUNK, :].astype(BF16)
    rows = []
    for p in range(2):
        rows.append(go(atp.at[p, 1 - core], ap.at[p], asend.at[p], arecv.at[p], twin))

    def part(p, k, lo, hi):
        first = PARTS[p][0]
        return wbuf.at[k, 0:CHUNK, first + lo:first + hi]

    def product(p, k):
        first, wide = PARTS[p]
        dest = (spots[p][0] + k) % 4
        cols = slice(first, first + wide)
        return nn(atp[p - 2, core, dest], yo[:, cols]) + nn(ap[p - 2, dest], yt[:, cols])

    relays = {}
    direct = {}

    def relay(p):
        wide = PARTS[p][1]
        h = wide // 2
        relays[p, 0].wait_recv()
        here = part(p, 1, 0, h)
        here[...] = (here[...].astype(F32) + rel[p][0].astype(F32)).astype(BF16)
        direct[p, 2] = go(here, rin[p].at[0, :, 0:h], s1.at[p - 2, 4], v1.at[p - 2, 4], axes[p][0](1))
        relays[p, 1].wait_recv()
        here = part(p, 3, h, wide)
        here[...] = (here[...].astype(F32) + rel[p][1].astype(F32)).astype(BF16)
        direct[p, 3] = go(here, rin[p].at[1, :, h:wide], s1.at[p - 2, 5], v1.at[p - 2, 5], axes[p][0](3))

    def heads_back(grp, first=0, last=PER_KV):
        def backward(j, carry):
            h = grp * PER_KV + j
            gh = g[h]
            dot = jnp.sum(gh.astype(F32) * attn[h].astype(F32), axis=1, keepdims=True)
            dp = nt(gh, values_of(grp))
            dsc = (ws[h].astype(F32) * (dp - dot)).astype(BF16)
            ds[j] = dsc
            dq = nn(dsc, keys_of(grp)) * SCALE
            cols = pl.ds(pl.multiple_of(h * HEAD, HEAD), HEAD)
            dqp[:, cols] = dq[0:PROMPT]
            dql[:, cols] = dq[PROMPT:ROWS]
            return carry

        lax.fori_loop(first, last, backward, 0)

    def keys_back(grp):
        stack = slice(grp * PER_KV, (grp + 1) * PER_KV)
        tall = PER_KV * ROWS
        dk = tn(qs[stack].reshape(tall, HEAD), ds[...].reshape(tall, KEYS)) * SCALE
        dkv[grp, :, :, 0:HEAD] = dk.T.astype(BF16).reshape(PEERS, ROWS, HEAD)
        dv = tn(g[stack].reshape(tall, HEAD), ws[stack].reshape(tall, KEYS))
        dkv[grp, :, :, HEAD:256] = dv.T.astype(BF16).reshape(PEERS, ROWS, HEAD)

    def hop(grp, i, src, dst, device):
        return go(src, dst, ksend.at[grp, i], krecv.at[grp, i], device)

    hops = {}

    def add_in(grp, q, cols, i):
        here = dkv.at[grp, q, :, cols]
        here[...] = (here[...].astype(F32) + kin[grp, i, :, cols].astype(F32)).astype(BF16)

    left, right, whole = slice(0, HEAD), slice(HEAD, 256), slice(0, 256)

    def grads_one(grp):
        hops[grp, 0] = hop(grp, 0, dkv.at[grp, slot(1 - plane, 2)], kin.at[grp, 0], across)
        hops[grp, 1] = hop(grp, 1, dkv.at[grp, slot(1 - plane, 1)], kin.at[grp, 1], on_x(1))
        hops[grp, 2] = hop(grp, 2, dkv.at[grp, slot(1 - plane, 3)], kin.at[grp, 2], on_x(3))

    def grads_two(grp):
        hops[grp, 0].wait_recv()
        far = slot(plane, 2)
        add_in(grp, far, whole, 0)
        hops[grp, 3] = hop(grp, 3, dkv.at[grp, far, :, left], kin.at[grp, 3, :, left], on_x(1))
        hops[grp, 4] = hop(grp, 4, dkv.at[grp, far, :, right], kin.at[grp, 3, :, right], on_x(3))
        hops[grp, 1].wait_recv()
        hops[grp, 2].wait_recv()
        near = slot(1 - plane, 0)
        total = dkv[grp, near].astype(F32) + kin[grp, 1].astype(F32) + kin[grp, 2].astype(F32)
        dkv[grp, near] = total.astype(BF16)
        hops[grp, 7] = hop(grp, 7, dkv.at[grp, near], kin.at[grp, 4], across)

    def grads_three(grp):
        hops[grp, 3].wait_recv()
        add_in(grp, slot(plane, 1), left, 3)
        hops[grp, 5] = hop(grp, 5, dkv.at[grp, slot(plane, 1)], kin.at[grp, 5], on_x(1))
        hops[grp, 4].wait_recv()
        add_in(grp, slot(plane, 3), right, 3)
        hops[grp, 6] = hop(grp, 6, dkv.at[grp, slot(plane, 3)], kin.at[grp, 6], on_x(3))

    def grads_last(grp):
        total = dkv[grp, seq].astype(F32)
        for i in (7, 5, 6):
            hops[grp, i].wait_recv()
        for i in (4, 5, 6):
            total = total + kin[grp, i].astype(F32)
        dkv_out[:, grp * HEAD:(grp + 1) * HEAD] = total[:, 0:HEAD]
        dkv_out[:, 256 + grp * HEAD:256 + (grp + 1) * HEAD] = total[:, HEAD:256]

    second = {}
    third = {}

    def send_second(p, pieces):
        pad = jnp.zeros((8, PARTS[p][1]), F32)
        for j in range(4):
            b2[p][j] = jnp.concatenate([pieces[j], pad], axis=0).astype(BF16)
        spot = spots[p][1]
        for k in (2, 1, 3):
            second[p, k] = go(b2[p].at[(spot + k) % 4], r2[p].at[k - 1], s2.at[p, k - 1], v2.at[p, k - 1], axes[p][1](k))

    def gathered(p):
        first, wide = PARTS[p]
        cols = slice(first, first + wide)
        full = nn(atn[core, y], yo[:, cols]) + nn(ag[0, 1 - core], yt[:, cols])
        for k in (1, 3, 2):
            for c in range(2):
                full = full + nn(ag[k, c], yg[k - 1, c, :, cols])
        if p == 0:
            send_second(p, [full[j * 56:(j + 1) * 56] for j in range(4)])
        else:
            strips = []
            for j in range(4):
                rows_of = [full[zz * 56 + j * SHARE:zz * 56 + (j + 1) * SHARE] for zz in range(4)]
                strips.append(jnp.concatenate(rows_of, axis=0))
            send_second(p, strips)

    def scattered(p):
        for i in range(4):
            direct[p, i].wait_recv()
        pieces = []
        for j in range(4):
            piece = slice(j * 56, (j + 1) * 56)
            pieces.append(own[p][piece] + rin[p][0, piece].astype(F32) + rin[p][1, piece].astype(F32))
        send_second(p, pieces)

    def send_third(p):
        for k in (1, 2, 3):
            second[p, k].wait_recv()
        full = b2[p][spots[p][1]].astype(F32)
        for k in range(3):
            full = full + r2[p][k].astype(F32)
        pad = jnp.zeros((2, PARTS[p][1]), F32)
        for j in range(4):
            piece = full[j * SHARE:(j + 1) * SHARE]
            b3[p][j] = jnp.concatenate([piece, pad], axis=0).astype(BF16)
        spot = spots[p][2]
        for k in (2, 1, 3):
            third[p, k] = go(b3[p].at[(spot + k) % 4], r3[p].at[k - 1], s3.at[p, k - 1], v3.at[p, k - 1], axes[p][2](k))

    heads_back(0, 0, 3)
    for c in swaps:
        c.wait_recv()
    for c in rows:
        c.wait_recv()
    for p in (2, 3):
        wide = PARTS[p][1]
        h = wide // 2
        part(p, 2, 0, wide)[...] = product(p, 2).astype(BF16)
        relays[p, 0] = go(part(p, 2, 0, h), rel[p].at[0], s1.at[p - 2, 0], v1.at[p - 2, 0], axes[p][0](1))
        relays[p, 1] = go(part(p, 2, h, wide), rel[p].at[1], s1.at[p - 2, 1], v1.at[p - 2, 1], axes[p][0](3))
    for p in (2, 3):
        wide = PARTS[p][1]
        h = wide // 2
        part(p, 1, 0, wide)[...] = product(p, 1).astype(BF16)
        direct[p, 0] = go(part(p, 1, h, wide), rin[p].at[0, :, h:wide], s1.at[p - 2, 2], v1.at[p - 2, 2], axes[p][0](1))
        part(p, 3, 0, wide)[...] = product(p, 3).astype(BF16)
        direct[p, 1] = go(part(p, 3, 0, h), rin[p].at[1, :, 0:h], s1.at[p - 2, 3], v1.at[p - 2, 3], axes[p][0](3))
    for p in (2, 3):
        own[p][...] = product(p, 0)
    heads_back(0, 3, PER_KV)
    keys_back(0)
    grads_one(0)
    came(yg.at[1, core, :, lower], 4)
    came(yg.at[1, core, :, upper], 5)
    strip(yg.at[1, core], yg.at[1, core], 8, twin)
    relay(2)
    relay(3)
    heads_back(1)
    send_to(ag.at[0, 1 - core], ag.at[0, 1 - core], esend.at[0, 0], erecv.at[0, 1 - core], twin).wait_recv()
    for k in (1, 2, 3):
        for c in range(2):
            send_to(ag.at[k, c], ag.at[k, c], esend.at[k, c], erecv.at[k, c], twin).wait_recv()
    came(yg.at[2, 1 - core], 6)
    came(yg.at[0, 1 - core], 7)
    came(yg.at[1, 1 - core], 8)
    gathered(0)
    gathered(1)
    keys_back(1)
    grads_one(1)
    grads_two(0)
    scattered(2)
    scattered(3)
    grads_two(1)
    grads_three(0)
    send_third(0)
    send_third(1)
    grads_three(1)
    send_third(2)
    send_third(3)
    grads_last(0)
    for p in range(4):
        first, wide = PARTS[p]
        for k in (1, 2, 3):
            third[p, k].wait_recv()
        full = b3[p][spots[p][2]].astype(F32)
        for k in range(3):
            full = full + r3[p][k].astype(F32)
        wg[:, first:first + wide] = full[0:SHARE] * (1.0 / math.sqrt(TOKENS))
    grads_last(1)
    for c in started:
        c.wait_send()


def tree_call(pq, pk, pv, lq, lk, lv, pdy, ldy, w, lengths, offsets, parents):
    any_ = pl.BlockSpec(memory_space=pl.ANY)
    vm = pl.BlockSpec(memory_space=VMEM)
    sm = pl.BlockSpec(memory_space=SMEM)
    widths = [wide for _, wide in PARTS]
    dma = pltpu.SemaphoreType.DMA
    scratch = [
        pltpu.VMEM((PEERS, ROWS, 512), BF16),
        pltpu.VMEM((ROWS, D), BF16),
        pltpu.VMEM((ROWS, D), BF16),
        pltpu.VMEM((WIDTH // 256, 256, D), BF16),
        pltpu.VMEM((HEADS, ROWS, HEAD), BF16),
        pltpu.VMEM((HEADS, ROWS, HEAD), BF16),
        pltpu.VMEM((HEADS, ROWS, HEAD), BF16),
        pltpu.VMEM((HEADS, ROWS, KEYS), BF16),
        pltpu.VMEM((PER_KV, ROWS, KEYS), BF16),
        pltpu.VMEM((WIDTH, ROWS), F32),
        pltpu.VMEM((2, 4 * CHUNK, ROWS), F32),
        pltpu.VMEM((2, 4, CHUNK, ROWS), BF16),
        pltpu.VMEM((2, 2, 4, CHUNK, ROWS), BF16),
        pltpu.VMEM((2, 4, CHUNK, ROWS), BF16),
        pltpu.VMEM((4, 2, CHUNK, ROWS), BF16),
        pltpu.VMEM((3, 2, ROWS, GATHERED), BF16),
        pltpu.VMEM((ROWS, KEYS), F32),
        pltpu.VMEM((GROUPS, PEERS, ROWS, 256), BF16),
        pltpu.VMEM((GROUPS, 7, ROWS, 256), BF16),
        pltpu.VMEM((ROWS, KEYS), F32),
        pltpu.VMEM((ROWS, KEYS), F32),
    ]
    late = widths[2:]
    scratch += [pltpu.VMEM((CHUNK, wide), F32) for wide in late]
    scratch += [pltpu.VMEM((2, CHUNK, wide // 2), BF16) for wide in late]
    scratch += [pltpu.VMEM((2, CHUNK, wide), BF16) for wide in late]
    scratch += [pltpu.VMEM((4, 64, wide), BF16) for wide in widths]
    scratch += [pltpu.VMEM((3, 64, wide), BF16) for wide in widths]
    scratch += [pltpu.VMEM((4, 16, wide), BF16) for wide in widths]
    scratch += [pltpu.VMEM((3, 16, wide), BF16) for wide in widths]
    scratch += [dma((4,)), dma((2,)), dma((WIDTH // 256,)), dma((HEADS, 2)), dma((10,)), dma((10,))]
    scratch += [dma((2,)), dma((2,)), dma((9,)), dma((9,)), dma((4, 2)), dma((4, 2)), dma((2,)), dma((2,))]
    scratch += [dma((GROUPS, 8)), dma((GROUPS, 8)), dma((2, 6)), dma((2, 6))]
    scratch += [dma((4, 3)), dma((4, 3)), dma((4, 3)), dma((4, 3))]
    return pl.pallas_call(
        tree_kernel,
        out_shape=(
            jax.ShapeDtypeStruct((PROMPT, WIDTH), F32),
            jax.ShapeDtypeStruct((LEAF, WIDTH), F32),
            jax.ShapeDtypeStruct((SHARE, D), F32),
            jax.ShapeDtypeStruct((ROWS, 512), F32),
        ),
        in_specs=[any_] * 9 + [sm] * 3,
        out_specs=(vm,) * 4,
        scratch_shapes=scratch,
        compiler_params=pltpu.CompilerParams(
            collective_id=0, has_side_effects=True, vmem_limit_bytes=LIMIT
        ),
        name="tree",
    )(pq, pk, pv, lq, lk, lv, pdy, ldy, w, lengths, offsets, parents)


def finish_kernel(dqp, dql, wg, dkv, pdq, pdk, pdv, ldq, ldk, ldv, out):
    pdq[...] = dqp[...]
    ldq[...] = dql[...]
    pdk[...] = dkv[0:PROMPT, 0:256]
    pdv[...] = dkv[0:PROMPT, 256:512]
    ldk[...] = dkv[PROMPT:ROWS, 0:256]
    ldv[...] = dkv[PROMPT:ROWS, 256:512]
    out[...] = wg[...]


def finish_call(dqp, dql, wg, dkv):
    vm = pl.BlockSpec(memory_space=VMEM)
    return pl.pallas_call(
        finish_kernel,
        out_shape=(
            jax.ShapeDtypeStruct((PROMPT, WIDTH), F32),
            jax.ShapeDtypeStruct((PROMPT, 256), F32),
            jax.ShapeDtypeStruct((PROMPT, 256), F32),
            jax.ShapeDtypeStruct((LEAF, WIDTH), F32),
            jax.ShapeDtypeStruct((LEAF, 256), F32),
            jax.ShapeDtypeStruct((LEAF, 256), F32),
            jax.ShapeDtypeStruct((SHARE, D), F32),
        ),
        in_specs=[vm] * 4,
        out_specs=(vm,) * 7,
        name="finish",
    )(dqp, dql, wg, dkv)


def body(pq, pk, pv, lq, lk, lv, pdy, ldy, w, lengths, offsets, parents):
    done = tree_call(
        pq[0], pk[0], pv[0], lq[0], lk[0], lv[0], pdy[0], ldy[0], w, lengths, offsets, parents
    )
    outs = finish_call(*done)
    return tuple(o[None] for o in outs[0:6]) + (outs[6],)


def solution(mesh):
    rows = P("leaf", "seq", None)
    placed = (rows,) * 8 + (P(),) + (P("leaf", None),) * 3
    return jax.shard_map(
        body,
        mesh=mesh,
        in_specs=placed,
        out_specs=(rows,) * 6 + (P(("leaf", "seq"), None),),
        check_vma=False,
    )
```

```python
import math

import jax
import jax.numpy as jnp
from jax import lax
from jax.experimental import pallas as pl
from jax.experimental.pallas import tpu as pltpu
from jax.sharding import PartitionSpec as P

MESH = pl.DeviceIdType.MESH
HEAD = 128
HEADS = 14
GROUPS = 2
PER_KV = 7
WIDTH = HEADS * HEAD
D = 3584
PROMPT = 128
LEAF = 48
ROWS = PROMPT + LEAF
PEERS = 8
KEYS = PEERS * ROWS
TOKENS = 16 * KEYS
SHARE = 14
BRANCHES = 16
CHUNK = 16 * SHARE
SCALE = 1.0 / math.sqrt(HEAD)
LOG2E = 1.0 / math.log(2.0)
NEG = -1e30
HALF_ROWS = CHUNK // 2
GATHERED = 2048
PARTS = ((0, 1024), (1024, 1024), (2048, 768), (2816, 768))
VMEM = pltpu.MemorySpace.VMEM
SMEM = pltpu.MemorySpace.SMEM
HALF = 256
LIMIT = 63 * 1024 * 1024
F32 = jnp.float32
BF16 = jnp.bfloat16


def nt(a, b):
    return lax.dot_general(a, b, (((1,), (1,)), ((), ())), preferred_element_type=F32)


def nn(a, b):
    return lax.dot_general(a, b, (((1,), (0,)), ((), ())), preferred_element_type=F32)


def tn(a, b):
    return lax.dot_general(a, b, (((0,), (0,)), ((), ())), preferred_element_type=F32)


def send_to(src, dst, send_sem, recv_sem, device):
    return pltpu.make_async_remote_copy(
        src_ref=src,
        dst_ref=dst,
        send_sem=send_sem,
        recv_sem=recv_sem,
        device_id=device,
        device_id_type=MESH,
    )


def flip(value, bit):
    low = (value // bit) % 2
    return value + bit - 2 * bit * low


def seq_peers(seq):
    found = []
    for d in range(1, PEERS):
        p = seq
        for bit in (1, 2, 4):
            if d & bit:
                p = flip(p, bit)
        found.append(p)
    return found


def visibility(lengths, offsets, parents, seq, bias):
    rows = lax.broadcasted_iota(jnp.int32, (ROWS, 1), 0)
    is_leaf = rows >= PROMPT
    query = jnp.where(is_leaf, seq * LEAF + rows - PROMPT, seq * PROMPT + rows)
    cols = lax.broadcasted_iota(jnp.int32, (1, KEYS), 1)
    slot = jnp.zeros((1, KEYS), jnp.int32)
    for s in range(1, PEERS):
        slot = slot + (cols >= s * ROWS).astype(jnp.int32)
    spot = cols - slot * ROWS
    key_leaf = spot >= PROMPT
    key = jnp.where(key_leaf, slot * LEAF + spot - PROMPT, slot * PROMPT + spot)
    key_branch = jnp.zeros((1, KEYS), jnp.int32)
    query_branch = jnp.zeros((ROWS, 1), jnp.int32)
    end = jnp.int32(0)
    for b in range(BRANCHES):
        end = end + lengths[0, b]
        key_branch = key_branch + (key >= end).astype(jnp.int32)
        query_branch = query_branch + (query >= end).astype(jnp.int32)
    fork = jnp.zeros((ROWS, 1), jnp.int32)
    ancestor = jnp.zeros((ROWS, 1), jnp.int32)
    for b in range(BRANCHES):
        here = query_branch == b
        fork = jnp.where(here, offsets[0, b], fork)
        ancestor = jnp.where(here, parents[0, b], ancestor)
    ancestor = jnp.where(is_leaf & (ancestor != query_branch), ancestor, -1)
    branch = jnp.where(is_leaf, query_branch, -1)
    reach = jnp.where(is_leaf, fork, query + 1)
    prompt_key = jnp.where(key_leaf, 1 << 20, key)
    key_branch = jnp.where(key_leaf, key_branch, -2)
    sees = prompt_key < reach
    sees = sees | ((key_branch == branch) & (key <= query))
    sees = sees | (key_branch == ancestor)
    bias[...] = jnp.where(sees, 0.0, NEG)


def tree_kernel(
    pq, pk, pv, lq, lk, lv, pdy, ldy, w, lengths, offsets, parents,
    dqp_out, dql_out, wg, dkv_out, *scratch
):
    (kv, yo, yt, wbuf, g, qs, attn, ws, ds, at, perm, atn, atp, ap, ag, yg, bias, dkv, kin, sa, sb) = scratch[0:21]
    own = dict(zip((2, 3), scratch[21:23]))
    rel = dict(zip((2, 3), scratch[23:25]))
    rin = dict(zip((2, 3), scratch[25:27]))
    b2 = scratch[27:31]
    r2 = scratch[31:35]
    b3 = scratch[35:39]
    r3 = scratch[39:43]
    (lsem, dsem, wsem, qsem, gsend, grecv, ysend, yrecv, psend, precv, esend, erecv, asend, arecv,
     ksend, krecv, s1, v1, s2, v2, s3, v3, dqp, dql, osem) = scratch[43:]
    leaf = lax.axis_index("leaf")
    seq = lax.axis_index("seq")
    core = leaf % 2
    y = leaf // 4
    plane = seq // 4
    z = ((leaf // 2) % 2) * 2 + plane
    x = seq % 4
    twin = (flip(leaf, 1), seq)
    peers = seq_peers(seq)

    def slot(q, k):
        return q * 4 + (x + k) % 4

    def on_x(k):
        return (leaf, slot(plane, k))

    def on_y(k):
        return (((y + k) % 4) * 4 + leaf % 4, seq)

    def on_z(k):
        other = (z + k) % 4
        return (y * 4 + (other // 2) * 2 + core, (other % 2) * 4 + x)

    across = (leaf, slot(1 - plane, 0))
    def on_y_core(k, c):
        return (((y + k) % 4) * 4 + ((leaf // 2) % 2) * 2 + c, seq)

    axes = ((on_y, on_z, on_x), (on_y, on_x, on_z), (on_x, on_y, on_z), (on_z, on_y, on_x))
    spots = ((y, z, x), (y, x, z), (x, y, z), (z, y, x))

    mine = [
        pltpu.make_async_copy(pk, kv.at[seq, 0:PROMPT, 0:256], lsem.at[0]),
        pltpu.make_async_copy(pv, kv.at[seq, 0:PROMPT, 256:512], lsem.at[1]),
        pltpu.make_async_copy(lk, kv.at[seq, PROMPT:ROWS, 0:256], lsem.at[2]),
        pltpu.make_async_copy(lv, kv.at[seq, PROMPT:ROWS, 256:512], lsem.at[3]),
    ]
    for c in mine:
        c.start()
    ups = [
        pltpu.make_async_copy(pdy, yo.at[0:PROMPT], dsem.at[0]),
        pltpu.make_async_copy(ldy, yo.at[PROMPT:ROWS], dsem.at[1]),
    ]
    for c in ups:
        c.start()
    tiles = WIDTH // 256
    for t in range(tiles):
        pltpu.make_async_copy(w.at[t * 256:(t + 1) * 256], wbuf.at[t], wsem.at[t]).start()
    queries = []
    for h in range(HEADS):
        cols = slice(h * HEAD, (h + 1) * HEAD)
        queries.append(pltpu.make_async_copy(pq.at[:, cols], qs.at[h, 0:PROMPT], qsem.at[h, 0]))
        queries.append(pltpu.make_async_copy(lq.at[:, cols], qs.at[h, PROMPT:ROWS], qsem.at[h, 1]))
    for c in queries:
        c.start()
    barrier = pltpu.get_barrier_semaphore()
    greet = [(leaf, p) for p in peers] + [twin]
    greet += [on_y(k) for k in (1, 2, 3)] + [on_z(k) for k in (1, 2, 3)]
    greet += [on_y_core(k, 1 - core) for k in (1, 2, 3)]
    for d in greet:
        pl.semaphore_signal(barrier, inc=1, device_id=d, device_id_type=MESH)
    pl.semaphore_wait(barrier, len(greet))
    started = []

    def go(src, dst, send_sem, recv_sem, device):
        c = send_to(src, dst, send_sem, recv_sem, device)
        c.start()
        started.append(c)
        return c

    def pass_on(ref, i, device):
        return go(ref, ref, gsend.at[i], grecv.at[i], device)

    def arrived(ref, i):
        send_to(ref, ref, gsend.at[i], grecv.at[i], across).wait_recv()

    for c in mine:
        c.wait()
    block = kv.at[seq]
    pass_on(block, 0, across)
    pass_on(kv.at[seq, :, 0:HALF], 1, on_x(1))
    pass_on(kv.at[seq, :, HALF:512], 2, on_x(3))
    pass_on(kv.at[seq, :, HALF:512], 8, on_x(1))
    pass_on(kv.at[seq, :, 0:HALF], 9, on_x(3))
    swaps = [
        go(pdy, yt.at[0:PROMPT], ysend.at[0], yrecv.at[0], twin),
        go(ldy, yt.at[PROMPT:ROWS], ysend.at[1], yrecv.at[1], twin),
    ]
    for c in ups:
        c.wait()

    def strip(src, dst, i, device):
        return go(src, dst, psend.at[i], precv.at[i], device)

    def came(dst, i):
        send_to(dst, dst, psend.at[i], precv.at[i], twin).wait_recv()

    quarter = GATHERED // 2
    lower, upper = slice(0, quarter), slice(quarter, GATHERED)
    strip(yo.at[:, lower], yg.at[2, core, :, lower], 0, on_y(1))
    strip(yo.at[:, upper], yg.at[0, core, :, upper], 1, on_y(3))
    strip(yo.at[:, upper], yg.at[2, core, :, upper], 2, on_y(1))
    strip(yo.at[:, lower], yg.at[0, core, :, lower], 3, on_y(3))

    def tile(t, carry):
        pltpu.make_async_copy(w.at[0:256], wbuf.at[t], wsem.at[t]).wait()
        acc = nt(yo[...], wbuf[t]).astype(BF16)
        g[2 * t] = acc[:, 0:HEAD]
        g[2 * t + 1] = acc[:, HEAD:256]
        return carry

    lax.fori_loop(0, tiles, tile, 0)
    arrived(kv.at[slot(plane, 3), :, 0:HALF], 1)
    pass_on(kv.at[slot(plane, 3), :, 0:HALF], 3, on_x(1))
    arrived(kv.at[slot(plane, 1), :, HALF:512], 2)
    pass_on(kv.at[slot(plane, 1), :, HALF:512], 4, on_x(3))
    arrived(kv.at[slot(1 - plane, 0)], 0)
    pass_on(kv.at[slot(1 - plane, 0)], 5, on_x(1))
    pass_on(kv.at[slot(1 - plane, 0)], 6, on_x(3))
    visibility(lengths, offsets, parents, seq, bias)
    arrived(kv.at[slot(plane, 2), :, 0:HALF], 3)
    arrived(kv.at[slot(plane, 2), :, HALF:512], 4)
    pass_on(kv.at[slot(plane, 2)], 7, across)
    for c in queries:
        c.wait()
    came(yg.at[2, core, :, lower], 0)
    strip(yg.at[2, core, :, lower], yg.at[1, core, :, lower], 4, on_y(1))
    came(yg.at[0, core, :, upper], 1)
    strip(yg.at[0, core, :, upper], yg.at[1, core, :, upper], 5, on_y(3))
    arrived(kv.at[slot(plane, 3), :, HALF:512], 8)
    arrived(kv.at[slot(plane, 1), :, 0:HALF], 9)
    arrived(kv.at[slot(1 - plane, 3)], 5)
    arrived(kv.at[slot(1 - plane, 1)], 6)
    arrived(kv.at[slot(1 - plane, 2)], 7)

    def keys_of(grp):
        cols = pl.ds(pl.multiple_of(grp * HEAD, HEAD), HEAD)
        return kv[:, :, cols].reshape(KEYS, HEAD)

    def values_of(grp):
        cols = pl.ds(pl.multiple_of(256 + grp * HEAD, HEAD), HEAD)
        return kv[:, :, cols].reshape(KEYS, HEAD)

    def part(p, k, u, lo, hi):
        first = PARTS[p][0]
        return wbuf.at[k, HALF_ROWS * u:HALF_ROWS * (u + 1), first + lo:first + hi]

    def strips_of(u):
        return slice(HALF_ROWS * u, HALF_ROWS * (u + 1))

    def product(p, k, u):
        first, wide = PARTS[p]
        dest = (spots[p][0] + k) % 4
        cols = slice(first, first + wide)
        here = strips_of(u)
        return nn(atp[p - 2, core, dest, here], yo[:, cols]) + nn(ap[p - 2, dest, here], yt[:, cols])

    relays = {}
    direct = {}
    rows = {}

    def arrange(u):
        here = strips_of(u)
        for c in range(2):
            for yy in (2 * u, 2 * u + 1):
                for zz in range(4):
                    n = yy * 448 + (zz // 2) * 224 + c * 112 + (zz % 2) * 56
                    r = zz * CHUNK + yy * 56
                    perm[1, r:r + 56, :] = at[n:n + 56, :]
                    for xx in range(4):
                        r = xx * CHUNK + yy * 56 + zz * SHARE
                        perm[0, r:r + SHARE, :] = at[n + xx * SHARE:n + (xx + 1) * SHARE, :]
            for k in range(4):
                for p in range(2):
                    r = k * CHUNK + u * HALF_ROWS
                    atp[p, c, k, here] = perm[p, r:r + HALF_ROWS, :].astype(BF16)
        for p in range(2):
            rows[p, u] = go(atp.at[p, 1 - core, :, here], ap.at[p, :, here], asend.at[p, u], arecv.at[p, u], twin)

    def multiply(u):
        here = strips_of(u)
        for p in range(2):
            rows[p, u].wait_recv()
        for p in (2, 3):
            wide = PARTS[p][1]
            h = wide // 2
            n = p - 2
            part(p, 2, u, 0, wide)[...] = product(p, 2, u).astype(BF16)
            relays[p, u, 0] = go(part(p, 2, u, 0, h), rel[p].at[0, here], s1.at[n, u, 0], v1.at[n, u, 0], axes[p][0](1))
            relays[p, u, 1] = go(part(p, 2, u, h, wide), rel[p].at[1, here], s1.at[n, u, 1], v1.at[n, u, 1], axes[p][0](3))
        for p in (2, 3):
            wide = PARTS[p][1]
            h = wide // 2
            n = p - 2
            part(p, 1, u, 0, wide)[...] = product(p, 1, u).astype(BF16)
            direct[p, u, 0] = go(part(p, 1, u, h, wide), rin[p].at[0, here, h:wide], s1.at[n, u, 2], v1.at[n, u, 2], axes[p][0](1))
            part(p, 3, u, 0, wide)[...] = product(p, 3, u).astype(BF16)
            direct[p, u, 1] = go(part(p, 3, u, 0, h), rin[p].at[1, here, 0:h], s1.at[n, u, 3], v1.at[n, u, 3], axes[p][0](3))
        for p in (2, 3):
            own[p][here] = product(p, 0, u)

    def relay(p, u):
        wide = PARTS[p][1]
        h = wide // 2
        n = p - 2
        rows_of = strips_of(u)
        relays[p, u, 0].wait_recv()
        here = part(p, 1, u, 0, h)
        here[...] = (here[...].astype(F32) + rel[p][0, rows_of].astype(F32)).astype(BF16)
        direct[p, u, 2] = go(here, rin[p].at[0, rows_of, 0:h], s1.at[n, u, 4], v1.at[n, u, 4], axes[p][0](1))
        relays[p, u, 1].wait_recv()
        here = part(p, 3, u, h, wide)
        here[...] = (here[...].astype(F32) + rel[p][1, rows_of].astype(F32)).astype(BF16)
        direct[p, u, 3] = go(here, rin[p].at[1, rows_of, h:wide], s1.at[n, u, 5], v1.at[n, u, 5], axes[p][0](3))

    def score(h, out):
        out[...] = nt(qs[h], keys_of(h // PER_KV))

    def soften(h, src):
        for r in range(0, ROWS, 16):
            here = slice(r, r + 16)
            t = src[here] * (SCALE * LOG2E) + bias[here]
            e = jnp.exp2(t - jnp.max(t, axis=1, keepdims=True))
            share = 1.0 / jnp.sum(e, axis=1, keepdims=True)
            ws[h, here] = (e * share).astype(BF16)

    def attend(h):
        a = nn(ws[h], values_of(h // PER_KV)).astype(BF16)
        attn[h] = a
        at[pl.ds(pl.multiple_of(h * HEAD, HEAD), HEAD), :] = a.astype(F32).T

    def forward(i, carry):
        score(2 * i + 1, sb)
        soften(2 * i, sa)
        score(jnp.minimum(2 * i + 2, HEADS - 1), sa)
        attend(2 * i)
        soften(2 * i + 1, sb)
        attend(2 * i + 1)
        return carry

    score(0, sa)
    lax.fori_loop(0, 4, forward, 0)
    came(yg.at[2, core, :, upper], 2)
    strip(yg.at[2, core], yg.at[2, core], 6, twin)
    came(yg.at[0, core, :, lower], 3)
    strip(yg.at[0, core], yg.at[0, core], 7, twin)
    arrange(0)
    lax.fori_loop(4, 6, forward, 0)
    for c in swaps:
        c.wait_recv()
    multiply(0)
    lax.fori_loop(6, HEADS // 2, forward, 0)
    for c in range(2):
        for yy in range(4):
            for zh in range(2):
                n = yy * 448 + zh * 224 + c * 112
                atn[c, yy, zh * 112:(zh + 1) * 112, :] = at[n:n + 112, :].astype(BF16)
    for k in (2, 1, 3):
        for c in range(2):
            go(atn.at[c, (y + k) % 4], ag.at[4 - k, core], esend.at[k, c], erecv.at[4 - k, core], on_y_core(k, c))
    go(atn.at[1 - core, y], ag.at[0, core], esend.at[0, 0], erecv.at[0, core], twin)
    def heads_back(grp, first=0, last=PER_KV):
        def backward(j, carry):
            h = grp * PER_KV + j
            gh = g[h]
            dot = jnp.sum(gh.astype(F32) * attn[h].astype(F32), axis=1, keepdims=True)
            dp = nt(gh, values_of(grp))
            dsc = (ws[h].astype(F32) * (dp - dot)).astype(BF16)
            ds[j] = dsc
            dq = nn(dsc, keys_of(grp)) * SCALE
            cols = pl.ds(pl.multiple_of(h * HEAD, HEAD), HEAD)
            dqp[:, cols] = dq[0:PROMPT]
            dql[:, cols] = dq[PROMPT:ROWS]
            return carry

        lax.fori_loop(first, last, backward, 0)

    def keys_back(grp):
        stack = slice(grp * PER_KV, (grp + 1) * PER_KV)
        tall = PER_KV * ROWS
        dk = tn(qs[stack].reshape(tall, HEAD), ds[...].reshape(tall, KEYS)) * SCALE
        dkv[grp, :, :, 0:HEAD] = dk.T.astype(BF16).reshape(PEERS, ROWS, HEAD)
        dv = tn(g[stack].reshape(tall, HEAD), ws[stack].reshape(tall, KEYS))
        dkv[grp, :, :, HEAD:256] = dv.T.astype(BF16).reshape(PEERS, ROWS, HEAD)

    def hop(grp, i, src, dst, device):
        return go(src, dst, ksend.at[grp, i], krecv.at[grp, i], device)

    hops = {}

    def add_in(grp, q, cols, i):
        here = dkv.at[grp, q, :, cols]
        here[...] = (here[...].astype(F32) + kin[grp, i, :, cols].astype(F32)).astype(BF16)

    left, right, whole = slice(0, HEAD), slice(HEAD, 256), slice(0, 256)

    def grads_one(grp):
        hops[grp, 0] = hop(grp, 0, dkv.at[grp, slot(1 - plane, 2)], kin.at[grp, 0], across)
        hops[grp, 1] = hop(grp, 1, dkv.at[grp, slot(1 - plane, 1)], kin.at[grp, 1], on_x(1))
        hops[grp, 2] = hop(grp, 2, dkv.at[grp, slot(1 - plane, 3)], kin.at[grp, 2], on_x(3))

    def grads_two(grp):
        hops[grp, 0].wait_recv()
        far = slot(plane, 2)
        add_in(grp, far, whole, 0)
        hops[grp, 3] = hop(grp, 3, dkv.at[grp, far, :, left], kin.at[grp, 3, :, left], on_x(1))
        hops[grp, 4] = hop(grp, 4, dkv.at[grp, far, :, right], kin.at[grp, 3, :, right], on_x(3))
        hops[grp, 1].wait_recv()
        hops[grp, 2].wait_recv()
        near = slot(1 - plane, 0)
        total = dkv[grp, near].astype(F32) + kin[grp, 1].astype(F32) + kin[grp, 2].astype(F32)
        dkv[grp, near] = total.astype(BF16)
        hops[grp, 7] = hop(grp, 7, dkv.at[grp, near], kin.at[grp, 4], across)

    def grads_three(grp):
        hops[grp, 3].wait_recv()
        add_in(grp, slot(plane, 1), left, 3)
        hops[grp, 5] = hop(grp, 5, dkv.at[grp, slot(plane, 1)], kin.at[grp, 5], on_x(1))
        hops[grp, 4].wait_recv()
        add_in(grp, slot(plane, 3), right, 3)
        hops[grp, 6] = hop(grp, 6, dkv.at[grp, slot(plane, 3)], kin.at[grp, 6], on_x(3))

    def grads_last(grp):
        total = dkv[grp, seq].astype(F32)
        for i in (7, 5, 6):
            hops[grp, i].wait_recv()
        for i in (4, 5, 6):
            total = total + kin[grp, i].astype(F32)
        dkv_out[:, grp * HEAD:(grp + 1) * HEAD] = total[:, 0:HEAD]
        dkv_out[:, 256 + grp * HEAD:256 + (grp + 1) * HEAD] = total[:, HEAD:256]

    second = {}
    third = {}

    def send_second(p, pieces):
        pad = jnp.zeros((8, PARTS[p][1]), F32)
        for j in range(4):
            b2[p][j] = jnp.concatenate([pieces[j], pad], axis=0).astype(BF16)
        spot = spots[p][1]
        for k in (2, 1, 3):
            second[p, k] = go(b2[p].at[(spot + k) % 4], r2[p].at[k - 1], s2.at[p, k - 1], v2.at[p, k - 1], axes[p][1](k))

    def gathered(p):
        first, wide = PARTS[p]
        cols = slice(first, first + wide)
        full = nn(atn[core, y], yo[:, cols]) + nn(ag[0, 1 - core], yt[:, cols])
        for k in (1, 3, 2):
            for c in range(2):
                full = full + nn(ag[k, c], yg[k - 1, c, :, cols])
        if p == 0:
            send_second(p, [full[j * 56:(j + 1) * 56] for j in range(4)])
        else:
            strips = []
            for j in range(4):
                rows_of = [full[zz * 56 + j * SHARE:zz * 56 + (j + 1) * SHARE] for zz in range(4)]
                strips.append(jnp.concatenate(rows_of, axis=0))
            send_second(p, strips)

    def scattered(p):
        for u in range(2):
            for i in range(4):
                direct[p, u, i].wait_recv()
        pieces = []
        for j in range(4):
            piece = slice(j * 56, (j + 1) * 56)
            pieces.append(own[p][piece] + rin[p][0, piece].astype(F32) + rin[p][1, piece].astype(F32))
        send_second(p, pieces)

    def send_third(p):
        for k in (1, 2, 3):
            second[p, k].wait_recv()
        full = b2[p][spots[p][1]].astype(F32)
        for k in range(3):
            full = full + r2[p][k].astype(F32)
        pad = jnp.zeros((2, PARTS[p][1]), F32)
        for j in range(4):
            piece = full[j * SHARE:(j + 1) * SHARE]
            b3[p][j] = jnp.concatenate([piece, pad], axis=0).astype(BF16)
        spot = spots[p][2]
        for k in (2, 1, 3):
            third[p, k] = go(b3[p].at[(spot + k) % 4], r3[p].at[k - 1], s3.at[p, k - 1], v3.at[p, k - 1], axes[p][2](k))

    arrange(1)
    heads_back(0, 0, 3)
    multiply(1)
    relay(2, 0)
    relay(3, 0)
    heads_back(0, 3, PER_KV)
    keys_back(0)
    grads_one(0)
    relay(2, 1)
    relay(3, 1)
    came(yg.at[1, core, :, lower], 4)
    came(yg.at[1, core, :, upper], 5)
    strip(yg.at[1, core], yg.at[1, core], 8, twin)
    heads_back(1)
    outs = [
        pltpu.make_async_copy(dqp, dqp_out, osem.at[0]),
        pltpu.make_async_copy(dql, dql_out, osem.at[1]),
    ]
    for c in outs:
        c.start()
    keys_back(1)
    grads_one(1)
    grads_two(0)
    send_to(ag.at[0, 1 - core], ag.at[0, 1 - core], esend.at[0, 0], erecv.at[0, 1 - core], twin).wait_recv()
    for k in (1, 2, 3):
        for c in range(2):
            send_to(ag.at[k, c], ag.at[k, c], esend.at[k, c], erecv.at[k, c], twin).wait_recv()
    came(yg.at[2, 1 - core], 6)
    came(yg.at[0, 1 - core], 7)
    came(yg.at[1, 1 - core], 8)
    gathered(0)
    gathered(1)
    grads_three(0)
    grads_two(1)
    scattered(2)
    scattered(3)
    grads_three(1)
    send_third(0)
    send_third(1)
    grads_last(0)
    send_third(2)
    send_third(3)
    grads_last(1)
    for p in range(4):
        first, wide = PARTS[p]
        for k in (1, 2, 3):
            third[p, k].wait_recv()
        full = b3[p][spots[p][2]].astype(F32)
        for k in range(3):
            full = full + r3[p][k].astype(F32)
        wg[:, first:first + wide] = full[0:SHARE] * (1.0 / math.sqrt(TOKENS))
    for c in outs:
        c.wait()
    for c in started:
        c.wait_send()


def tree_call(pq, pk, pv, lq, lk, lv, pdy, ldy, w, lengths, offsets, parents):
    any_ = pl.BlockSpec(memory_space=pl.ANY)
    vm = pl.BlockSpec(memory_space=VMEM)
    sm = pl.BlockSpec(memory_space=SMEM)
    widths = [wide for _, wide in PARTS]
    dma = pltpu.SemaphoreType.DMA
    scratch = [
        pltpu.VMEM((PEERS, ROWS, 512), BF16),
        pltpu.VMEM((ROWS, D), BF16),
        pltpu.VMEM((ROWS, D), BF16),
        pltpu.VMEM((WIDTH // 256, 256, D), BF16),
        pltpu.VMEM((HEADS, ROWS, HEAD), BF16),
        pltpu.VMEM((HEADS, ROWS, HEAD), BF16),
        pltpu.VMEM((HEADS, ROWS, HEAD), BF16),
        pltpu.VMEM((HEADS, ROWS, KEYS), BF16),
        pltpu.VMEM((PER_KV, ROWS, KEYS), BF16),
        pltpu.VMEM((WIDTH, ROWS), F32),
        pltpu.VMEM((2, 4 * CHUNK, ROWS), F32),
        pltpu.VMEM((2, 4, CHUNK, ROWS), BF16),
        pltpu.VMEM((2, 2, 4, CHUNK, ROWS), BF16),
        pltpu.VMEM((2, 4, CHUNK, ROWS), BF16),
        pltpu.VMEM((4, 2, CHUNK, ROWS), BF16),
        pltpu.VMEM((3, 2, ROWS, GATHERED), BF16),
        pltpu.VMEM((ROWS, KEYS), F32),
        pltpu.VMEM((GROUPS, PEERS, ROWS, 256), BF16),
        pltpu.VMEM((GROUPS, 7, ROWS, 256), BF16),
        pltpu.VMEM((ROWS, KEYS), F32),
        pltpu.VMEM((ROWS, KEYS), F32),
    ]
    late = widths[2:]
    scratch += [pltpu.VMEM((CHUNK, wide), F32) for wide in late]
    scratch += [pltpu.VMEM((2, CHUNK, wide // 2), BF16) for wide in late]
    scratch += [pltpu.VMEM((2, CHUNK, wide), BF16) for wide in late]
    scratch += [pltpu.VMEM((4, 64, wide), BF16) for wide in widths]
    scratch += [pltpu.VMEM((3, 64, wide), BF16) for wide in widths]
    scratch += [pltpu.VMEM((4, 16, wide), BF16) for wide in widths]
    scratch += [pltpu.VMEM((3, 16, wide), BF16) for wide in widths]
    scratch += [dma((4,)), dma((2,)), dma((WIDTH // 256,)), dma((HEADS, 2)), dma((10,)), dma((10,))]
    scratch += [dma((2,)), dma((2,)), dma((9,)), dma((9,)), dma((4, 2)), dma((4, 2)), dma((2, 2)), dma((2, 2))]
    scratch += [dma((GROUPS, 8)), dma((GROUPS, 8)), dma((2, 2, 6)), dma((2, 2, 6))]
    scratch += [dma((4, 3)), dma((4, 3)), dma((4, 3)), dma((4, 3))]
    scratch += [pltpu.VMEM((PROMPT, WIDTH), F32), pltpu.VMEM((LEAF, WIDTH), F32), dma((2,))]
    return pl.pallas_call(
        tree_kernel,
        out_shape=(
            jax.ShapeDtypeStruct((PROMPT, WIDTH), F32),
            jax.ShapeDtypeStruct((LEAF, WIDTH), F32),
            jax.ShapeDtypeStruct((SHARE, D), F32),
            jax.ShapeDtypeStruct((ROWS, 512), F32),
        ),
        in_specs=[any_] * 9 + [sm] * 3,
        out_specs=(any_, any_, vm, vm),
        scratch_shapes=scratch,
        compiler_params=pltpu.CompilerParams(
            collective_id=0, has_side_effects=True, vmem_limit_bytes=LIMIT
        ),
        name="tree",
    )(pq, pk, pv, lq, lk, lv, pdy, ldy, w, lengths, offsets, parents)


def finish_kernel(dqp, dql, wg, dkv, pdq, pdk, pdv, ldq, ldk, ldv, out):
    pdq[...] = dqp[...]
    ldq[...] = dql[...]
    pdk[...] = dkv[0:PROMPT, 0:256]
    pdv[...] = dkv[0:PROMPT, 256:512]
    ldk[...] = dkv[PROMPT:ROWS, 0:256]
    ldv[...] = dkv[PROMPT:ROWS, 256:512]
    out[...] = wg[...]


def finish_call(dqp, dql, wg, dkv):
    vm = pl.BlockSpec(memory_space=VMEM)
    return pl.pallas_call(
        finish_kernel,
        out_shape=(
            jax.ShapeDtypeStruct((PROMPT, WIDTH), F32),
            jax.ShapeDtypeStruct((PROMPT, 256), F32),
            jax.ShapeDtypeStruct((PROMPT, 256), F32),
            jax.ShapeDtypeStruct((LEAF, WIDTH), F32),
            jax.ShapeDtypeStruct((LEAF, 256), F32),
            jax.ShapeDtypeStruct((LEAF, 256), F32),
            jax.ShapeDtypeStruct((SHARE, D), F32),
        ),
        in_specs=[vm] * 4,
        out_specs=(vm,) * 7,
        name="finish",
    )(dqp, dql, wg, dkv)


def body(pq, pk, pv, lq, lk, lv, pdy, ldy, w, lengths, offsets, parents):
    done = tree_call(
        pq[0], pk[0], pv[0], lq[0], lk[0], lv[0], pdy[0], ldy[0], w, lengths, offsets, parents
    )
    outs = finish_call(*done)
    return tuple(o[None] for o in outs[0:6]) + (outs[6],)


def solution(mesh):
    rows = P("leaf", "seq", None)
    placed = (rows,) * 8 + (P(),) + (P("leaf", None),) * 3
    return jax.shard_map(
        body,
        mesh=mesh,
        in_specs=placed,
        out_specs=(rows,) * 6 + (P(("leaf", "seq"), None),),
        check_vma=False,
    )
```
